32 devices in a mesh: blk: 8 (over y, x, core), lvl: 4 (over z).
Axes of the slice: x: 2, y: 2, z: 4, core: 2. Of those that a mesh axis runs over, the one named last changes fastest.
Arguments:
- vorticity: bfloat16 [4, 3, 64, 32768], P('lvl', None, 'blk'), may hold values from -6 to 6
- shift_field: bfloat16 [4, 64, 32768], P('lvl', 'blk'), may hold values from -0.8984375 to 0.8984375
- new_index: int32 [4, 64], P('lvl', 'blk'), may hold values from 0 to 63, as said below
- parent_slot: int32 [4, 64], P('lvl', 'blk'), may hold values from 0 to 511, as said below
- flags: int32 [4, 64], P('lvl', 'blk'), may hold values 0 or 1
Outputs:
- field: bfloat16 [4, 3, 64, 32768], P('lvl', None, 'blk')
The draws below stay inside these ranges and needn't reach their ends.
Inputs may be any that keep to these rules, and one draw needn't show every extreme that they name: `new_index`: in each level a permutation of the block positions; position b lies on device b // 8 of blk. No device sends more than 2 of its blocks to one device, and that number is reached. `parent_slot`: in each level all values differ; value // 8 is a block of the next coarser level and lies on device value // 64. No device has more than 2 blocks whose parents lie on one device, counting the blocks it holds before migration or those it holds after, and that number is reached in both. The values of level 0 are not used.
All inputs are finite; a program needn't handle non-finite values. No bound on the sum of `flags` on one device may be relied on, other than what follows from the above.
Results may differ from the reference program's by a relative error of at most 0.001.
Values may be sent and summed in bfloat16 or wider, within the bound.
A program may use at most 128 MiB of HBM per device.

```python
import jax
import jax.numpy as jnp

EDGE = 32
CELLS = 32768
B_DEV = 8
CAP = 2
BLOCKS = 64
N_BLK = 8
N_LVL = 4


def joint_routes(key):
    new_levels = []
    parent_levels = []
    for level in range(N_LVL):
        level_key = jax.random.fold_in(key, level)
        placing = jax.random.permutation(jax.random.fold_in(level_key, 1), N_BLK)
        inverse = jnp.zeros((N_BLK,), jnp.int32).at[placing].set(jnp.arange(N_BLK, dtype=jnp.int32))
        offsets = jax.random.permutation(jax.random.fold_in(level_key, 2), N_BLK)[:B_DEV // CAP]
        device_keys = jax.random.split(jax.random.fold_in(level_key, 3), N_BLK)
        shuffle = jax.vmap(lambda one: jax.random.permutation(one, B_DEV))(device_keys)
        groups = offsets[shuffle // CAP]
        target = (inverse[:, None] + groups) % N_BLK
        owners = placing[target]
        new_pos = (owners * B_DEV + shuffle).reshape(BLOCKS).astype(jnp.int32)
        parent_place = jax.random.permutation(jax.random.fold_in(level_key, 4), N_BLK)
        parent_dev = parent_place[(2 * inverse[:, None] + groups) % N_BLK].reshape(BLOCKS).astype(jnp.int32)
        onehot = (parent_dev[:, None] == jnp.arange(N_BLK, dtype=jnp.int32)[None, :]).astype(jnp.int32)
        rank = jnp.sum((jnp.cumsum(onehot, axis=0) - onehot) * onehot, axis=1).astype(jnp.int32)
        slot_keys = jax.random.split(jax.random.fold_in(level_key, 5), N_BLK)
        slots = jax.vmap(lambda one: jax.random.permutation(one, 8 * B_DEV))(slot_keys).astype(jnp.int32)
        value = parent_dev * (8 * B_DEV) + slots[parent_dev, rank]
        parent_at_new = jnp.zeros((BLOCKS,), jnp.int32).at[new_pos].set(value.astype(jnp.int32))
        new_levels.append(new_pos)
        parent_levels.append(parent_at_new)
    return (jnp.stack(new_levels, axis=0).astype(jnp.int32), jnp.stack(parent_levels, axis=0).astype(jnp.int32))


def draw_new_index(key, part):
    return joint_routes(jax.random.fold_in(key, 11))[0]


def draw_parent_slot(key, part):
    return joint_routes(jax.random.fold_in(key, 11))[1]


def set_ends(entries, stream_key, low, largest):
    longest = entries.shape.index(max(entries.shape))
    spots = []
    for shift in (0, 1):
        where = [jax.random.randint(jax.random.fold_in(stream_key, axis), (), 0, length) for axis, length in enumerate(entries.shape)]
        where[longest] = (where[longest] + shift) % entries.shape[longest]
        spots.append(tuple(where))
    return entries.at[spots[0]].set(low).at[spots[1]].set(largest)


def block_levels(rng, dims, cuts, least, top_value):
    loudness = 1.0
    for axis_at, shards_of in cuts:
        steps = jax.random.uniform(jax.random.fold_in(jax.random.fold_in(rng, 6), axis_at), (shards_of,), jnp.float32, least / len(cuts), top_value / len(cuts))
        loudness = loudness * jnp.repeat(jnp.exp(steps), dims[axis_at] // shards_of).reshape((-1,) + (1,) * (len(dims) - 1 - axis_at))
    return loudness


def centred(own_key, extent, width, most, shards=(), kind=jnp.bfloat16):
    factor_of = block_levels(own_key, extent, shards, -0.22, 0.18) if shards else 1.0
    array = jax.random.normal(own_key, extent, jnp.float32) * width * factor_of
    return jnp.minimum(jnp.maximum(array, -most), most).astype(kind)


def setup_inputs(seed: int = 0) -> dict:
    splits = jax.random.split(jax.random.key(seed), 6)
    return {
        "vorticity": centred(splits[0], (N_LVL, 3, BLOCKS, CELLS), 1.0, 6.0, ((0, 4), (2, 8))),
        "shift_field": jnp.clip(jax.random.uniform(splits[1], (N_LVL, BLOCKS, CELLS), jnp.float32, -0.8984375, 0.8984375) * block_levels(splits[1], (N_LVL, BLOCKS, CELLS), ((0, 4), (1, 8)), -0.4, 0.0), -0.8984375, 0.8984375).astype(jnp.bfloat16),
        "new_index": draw_new_index(jax.random.fold_in(splits[5], 71), 0),
        "parent_slot": draw_parent_slot(jax.random.fold_in(splits[5], 71), 0),
        "flags": set_ends((jax.random.randint(splits[4], (N_LVL, BLOCKS), 0, 2) < 1).astype(jnp.int32), jax.random.fold_in(splits[4], 1), 0, 1),
    }


def kernel_weight(distance):
    size = jnp.abs(distance)
    inner = 1.0 - 2.5 * size * size + 1.5 * size * size * size
    outer = 0.5 * (2.0 - size) * (2.0 - size) * (1.0 - size)
    return jnp.where(size < 1.0, inner, jnp.where(size < 2.0, outer, 0.0))


def deposit(values, shifts):
    total = None
    for offset in range(-2, 3):
        weight = kernel_weight(offset - shifts)
        term = values * weight[None]
        padded = jnp.pad(term, ((0, 0), (2 + offset, 2 - offset), (0, 0)))
        total = padded if total is None else total + padded
    return total


def assemble(coarse, marks, count):
    half = EDGE // 2
    full = coarse.reshape(3, count, 2, 2, 2, half, half, half)
    full = full.transpose(0, 1, 2, 5, 3, 6, 4, 7).reshape(3, count, CELLS)
    spread = marks.reshape(count, 2, 2, 2)[:, :, None, :, None, :, None]
    spread = jnp.broadcast_to(spread, (count, 2, half, 2, half, 2, half)).reshape(count, CELLS)
    return full, spread


def reference(vorticity, shift_field, new_index, parent_slot, flags):
    plane = EDGE * EDGE
    length = BLOCKS * EDGE
    half = EDGE // 2
    moved = []
    shrunk = []
    for level in range(N_LVL):
        chain_vort = vorticity[level].astype(jnp.float32).reshape(3, length, plane)
        chain_shift = shift_field[level].astype(jnp.float32).reshape(length, plane)
        remeshed = deposit(chain_vort, chain_shift)[:, 2:length + 2]
        remeshed = remeshed.astype(jnp.bfloat16).reshape(3, BLOCKS, CELLS)
        migrated = jnp.zeros_like(remeshed).at[:, new_index[level]].set(remeshed)
        moved.append(migrated)
        fine = migrated.astype(jnp.float32).reshape(3, BLOCKS, half, 2, half, 2, half, 2)
        shrunk.append((jnp.sum(fine, axis=(3, 5, 7)) * 0.125).reshape(3, BLOCKS, half * half * half))
    results = []
    for level in range(N_LVL):
        base = moved[level].astype(jnp.float32)
        if level + 1 < N_LVL:
            spots = jnp.where(flags[level + 1] == 1, parent_slot[level + 1], 8 * BLOCKS).astype(jnp.int32)
            coarse = jnp.zeros((3, 8 * BLOCKS + 1, half * half * half), jnp.float32)
            coarse = coarse.at[:, spots].set(shrunk[level + 1])[:, :8 * BLOCKS]
            marks = jnp.zeros((8 * BLOCKS + 1,), jnp.float32).at[spots].set(1.0)[:8 * BLOCKS]
            full, spread = assemble(coarse, marks, BLOCKS)
            base = jnp.where(spread[None] > 0.5, full, base)
        results.append(base.astype(jnp.bfloat16))
    return jnp.stack(results, axis=0)
```

```python
import functools

import jax
import jax.numpy as jnp
import numpy as np
from jax import lax
from jax.experimental import pallas as pl
from jax.experimental.pallas import tpu as pltpu
from jax.sharding import PartitionSpec as P

MESH = pl.DeviceIdType.MESH
EDGE = 32
PLANE = EDGE * EDGE
LANE_TILES = PLANE // 128
CAP = 2
SPAN = 8
ORDER = (1, 2, 0, 3)
VMEM_LIMIT = 60 * 1024 * 1024
PIECES = ((4 * PLANE, 20 * PLANE), (20 * PLANE, 32 * PLANE), (0, 4 * PLANE))


def device(blk, lvl):
    return {"blk": blk, "lvl": lvl}


def remote(src, dst, send, recv, target):
    return pltpu.make_async_remote_copy(
        src_ref=src, dst_ref=dst, send_sem=send, recv_sem=recv, device_id=target, device_id_type=MESH
    )


def tap_weights(shifts):
    size = jnp.abs(shifts)
    rest = 1.0 - size
    size2 = size * size
    rest2 = rest * rest
    middle = 1.0 + size2 * (1.5 * size - 2.5)
    ahead = 1.0 + rest2 * (1.5 * rest - 2.5)
    behind = -0.5 * rest2 * size
    far = -0.5 * size2 * rest
    up = shifts >= 0.0
    return {
        -2: jnp.where(up, 0.0, far),
        -1: jnp.where(up, behind, ahead),
        0: middle,
        1: jnp.where(up, ahead, behind),
        2: jnp.where(up, far, 0.0),
    }


def split(value, size):
    if size & (size - 1) == 0:
        return lax.shift_right_logical(value, size.bit_length() - 1), lax.bitwise_and(value, size - 1)
    return lax.div(value, size), lax.rem(value, size)


def picks(keys, wanted):
    count, first, second = jnp.int32(0), jnp.int32(0), jnp.int32(0)
    for b, key in enumerate(keys):
        hit = key == wanted
        first = jnp.where(jnp.logical_and(hit, count == 0), b, first)
        second = jnp.where(jnp.logical_and(hit, count == 1), b, second)
        count = count + hit.astype(jnp.int32)
    return first, second


def kernel(n, levels, spots_in, parents_in, flags_in, vort_in, shift_in, shrink_in, grow_in, out,
           spots, parent_slot, flags, field, shrink, grow,
           rows, patch, whole, masks, result,
           send0, send1, send2, send3, got0, got1, got2, got3,
           small, ghost, got_ghost,
           edge, edge_low, edge_high, below, above, halo_low, halo_high,
           tab, near_tabs, fine_tabs, near_local, fine_local, line, place, line2, octants,
           pick, pick_ghost,
           in_sem, index_sem, table_sem, halo_s, halo_r, near_s, near_r, coarse_s, coarse_r,
           block_s, block_r, ghost_s, ghost_r, out_sem, ready):
    me = lax.axis_index("blk")
    lvl = lax.axis_index("lvl")
    blocks = out.shape[1]
    spread = EDGE * LANE_TILES * blocks
    piece = SPAN * LANE_TILES
    coarse_level = jnp.maximum(lvl - 1, 0)
    fine_level = jnp.minimum(lvl + 1, levels - 1)
    sends, gots = (send0, send1, send2, send3), (got0, got1, got2, got3)
    after = device(lax.rem(me + 1, n), lvl)
    before = device(lax.rem(me + n - 1, n), lvl)
    has_coarse, has_fine = lvl > 0, lvl < levels - 1
    not_first, not_last = me > 0, me < n - 1

    barrier = pltpu.get_barrier_semaphore()

    def greet(blk, level):
        pl.semaphore_signal(barrier, inc=1, device_id=device(blk, level), device_id_type=MESH)

    for k in range(1, n):
        greet(lax.rem(me + k, n), lvl)

    @pl.when(has_coarse)
    def _():
        greet(me, coarse_level)

    @pl.when(has_fine)
    def _():
        greet(me, fine_level)

    index_loads = [
        pltpu.make_async_copy(src, dst, index_sem.at[i])
        for i, (src, dst) in enumerate(((spots_in, spots), (parents_in, parent_slot), (flags_in, flags)))
    ]
    loads = []
    for i, (lo, hi) in enumerate(PIECES):
        part = pl.ds(lo, hi - lo)
        loads.append((
            pltpu.make_async_copy(shift_in.at[:, part], field.at[3, :, part], in_sem.at[2 * i]),
            pltpu.make_async_copy(vort_in.at[:, :, part], field.at[pl.ds(0, 3), :, part], in_sem.at[2 * i + 1]),
        ))
    constants = (
        pltpu.make_async_copy(shrink_in, shrink, table_sem.at[0]),
        pltpu.make_async_copy(grow_in, grow, table_sem.at[1]),
    )
    for copy in index_loads:
        copy.start()
    for pair in loads:
        for copy in pair:
            copy.start()
    for copy in constants:
        copy.start()

    sublane = lax.broadcasted_iota(jnp.int32, (blocks, 128), 0)
    lane = lax.broadcasted_iota(jnp.int32, (1, 128), 1)

    def tile(f, x, j):
        at = pl.multiple_of(x * PLANE + j * 128, 128)
        return field[f, :, pl.ds(at, 128)].astype(jnp.float32)

    def source_tile(f, x, j):
        if x < 0:
            edge_row = halo_low[pl.ds(f * 16 + (x + 2) * LANE_TILES + j, 1), :]
            return jnp.where(sublane == 0, edge_row, pltpu.roll(tile(f, x + EDGE, j), 1, 0))
        if x >= EDGE:
            edge_row = halo_high[pl.ds(f * 16 + (x - EDGE) * LANE_TILES + j, 1), :]
            return jnp.where(sublane == blocks - 1, edge_row, pltpu.roll(tile(f, x - EDGE, j), blocks - 1, 0))
        return tile(f, x, j)

    def remesh(part):
        x0, x1 = part * SPAN, (part + 1) * SPAN

        def chunk(j, carry):
            sums = [{}, {}, {}]
            for x in range(x0 - 2, x1 + 2):
                weights = tap_weights(source_tile(3, x, j))
                for c in range(3):
                    value = source_tile(c, x, j)
                    for offset in range(-2, 3):
                        to = x + offset
                        if x0 <= to < x1:
                            term = value * weights[offset]
                            sums[c][to] = sums[c][to] + term if to in sums[c] else term
                    if x0 <= x - 2:
                        at = c * spread + ((x - 2) * LANE_TILES + j) * blocks
                        rows[pl.ds(pl.multiple_of(at, blocks), blocks), :] = sums[c].pop(x - 2)
            return carry

        lax.fori_loop(0, LANE_TILES, chunk, 0)
        for b in range(blocks):
            for c in range(3):
                at = c * spread + x0 * LANE_TILES * blocks + b
                whole[part, b, c * piece:(c + 1) * piece, :] = rows[
                    pl.ds(at, piece, stride=blocks), :
                ].astype(jnp.bfloat16)

    def pack(part):
        def one(k, carry):
            to = lax.rem(me + k, n)
            for s in range(CAP):
                sends[part][to, s] = whole[part, pick[CAP * to + s]]
            return carry

        lax.fori_loop(1, n, one, 0)

    def keep(part):
        for s in range(CAP):
            gots[part][CAP * me + s] = whole[part, pick[CAP * me + s]]

    def block_copy(part, k):
        to = lax.rem(me + k, n)
        return remote(sends[part].at[to], gots[part].at[pl.ds(CAP * me, CAP)],
                      block_s.at[part, k], block_r.at[part, k], device(to, lvl))

    def block_arrival(part, k):
        source = lax.rem(me + n - k, n)
        return remote(sends[part].at[me], gots[part].at[pl.ds(CAP * source, CAP)],
                      block_s.at[part, k], block_r.at[part, k], before)

    def send_blocks(part):
        for k in range(1, n):
            block_copy(part, k).start()

    def near(k):
        return remote(tab, near_tabs.at[me], near_s.at[k], near_r.at[k], device(lax.rem(me + k, n), lvl))

    def near_arrival(k):
        return remote(tab, near_tabs.at[lax.rem(me + n - k, n)], near_s.at[k], near_r.at[k], before)

    def coarse(k):
        return remote(tab, fine_tabs.at[me], coarse_s.at[k], coarse_r.at[k],
                      device(lax.rem(me + k, n), coarse_level))

    def coarse_arrival(k):
        return remote(tab, fine_tabs.at[lax.rem(me + n - k, n)], coarse_s.at[k], coarse_r.at[k], before)

    def ghost_copy(k):
        to = lax.rem(me + k, n)
        return remote(ghost.at[to], got_ghost.at[pl.ds(CAP * me, CAP)], ghost_s.at[k], ghost_r.at[k],
                      device(to, coarse_level))

    def ghost_arrival(k):
        source = lax.rem(me + n - k, n)
        return remote(ghost.at[me], got_ghost.at[pl.ds(CAP * source, CAP)], ghost_s.at[k], ghost_r.at[k], before)

    def high(target):
        return remote(edge_high, below, halo_s.at[0], halo_r.at[0], target)

    def low(target):
        return remote(edge_low, above, halo_s.at[1], halo_r.at[1], target)

    for copy in index_loads:
        copy.wait()
    head = jnp.zeros((1, 128), jnp.int32)
    for part, ref in enumerate((spots, parent_slot, flags)):
        for b in range(blocks):
            head = jnp.where(lane == part * blocks + b, ref[0, b], head)
    tab[...] = head
    near_tabs[me] = head
    owners = [split(spots[0, b], blocks)[0] for b in range(blocks)]

    def choose(to, carry):
        first, second = picks(owners, to)
        pick[CAP * to] = first
        pick[CAP * to + 1] = second
        return carry

    lax.fori_loop(0, n, choose, 0)

    for copy in loads[0]:
        copy.wait()
    remesh(ORDER[0])
    pack(ORDER[0])
    for copy in loads[1] + loads[2]:
        copy.wait()

    def edges(j, carry):
        for f in range(4):
            for p in range(2):
                at = f * 16 + p * LANE_TILES + j
                edge[pl.ds(at, 1), :] = tile(f, p, j)[0:1, :]
                edge[pl.ds(64 + at, 1), :] = tile(f, EDGE - 2 + p, j)[blocks - 1:blocks, :]
        return carry

    lax.fori_loop(0, LANE_TILES, edges, 0)
    edge_low[...] = edge[0:64, :].astype(jnp.bfloat16)
    edge_high[...] = edge[64:128, :].astype(jnp.bfloat16)

    nearby = n - 1 + has_coarse.astype(jnp.int32) + has_fine.astype(jnp.int32)
    pl.semaphore_wait(barrier, nearby)

    @pl.when(not_last)
    def _():
        high(after).start()

    @pl.when(not_first)
    def _():
        low(before).start()

    for k in range(1, n):
        near(k).start()
    send_blocks(ORDER[0])

    @pl.when(has_fine)
    def _():
        pl.semaphore_signal(ready, inc=1, device_id=device(me, fine_level), device_id_type=MESH)

    keep(ORDER[0])
    remesh(ORDER[1])
    pack(ORDER[1])
    send_blocks(ORDER[1])
    keep(ORDER[1])

    @pl.when(not_last)
    def _():
        low(after).wait_recv()

    @pl.when(not_first)
    def _():
        high(before).wait_recv()

    halo_low[...] = jnp.where(not_first, below[...].astype(jnp.float32), 0.0)
    halo_high[...] = jnp.where(not_last, above[...].astype(jnp.float32), 0.0)
    for part in ORDER[2:]:
        remesh(part)
        pack(part)
        send_blocks(part)
        keep(part)

    @pl.when(has_coarse)
    def _():
        pl.semaphore_wait(ready, 1)
        for k in range(n):
            coarse(k).start()

    for k in range(1, n):
        near_arrival(k).wait_recv()
    fetch_near = pltpu.make_async_copy(near_tabs, near_local, table_sem.at[2])
    fetch_near.start()
    fetch_near.wait()
    for copy in constants:
        copy.wait()

    @pl.when(has_coarse)
    def _():
        parents = []
        for b in range(blocks):
            home, spot = split(spots[0, b], blocks)
            parents.append(split(near_local[home, 0, blocks + spot], 8 * blocks)[0])

        def choose_ghost(to, carry):
            first, second = picks(parents, to)
            pick_ghost[CAP * to] = first
            pick_ghost[CAP * to + 1] = second
            return carry

        lax.fori_loop(0, n, choose_ghost, 0)

        def restrict(b, carry):
            columns = []
            for half in range(2):
                for dx in range(2):
                    for odd in range(2):
                        parts = []
                        for c in range(3):
                            for jj in range(4):
                                x, j = half * 16 + dx, 2 * jj + odd
                                at = c * spread + (x * LANE_TILES + j) * blocks + b
                                parts.append(rows[pl.ds(at, 8, stride=2 * LANE_TILES * blocks), :])
                        columns.append(jnp.concatenate(parts, axis=0).astype(jnp.bfloat16))
            wide = jnp.concatenate(columns, axis=1)
            small[b] = jnp.dot(wide, shrink[...], preferred_element_type=jnp.float32).astype(jnp.bfloat16)
            return carry

        lax.fori_loop(0, blocks, restrict, 0)

        def pack_ghost(to, carry):
            for s in range(CAP):
                ghost[to, s] = small[pick_ghost[CAP * to + s]]
            return carry

        lax.fori_loop(0, n, pack_ghost, 0)
        for k in range(n):
            ghost_copy(k).start()

    def settle_places(source, places):
        count = jnp.int32(0)
        for b in range(blocks):
            owner, spot = split(near_local[source, 0, b], blocks)
            mine = owner == me
            slot = CAP * source + jnp.minimum(count, CAP - 1)
            places = jnp.where(lane == jnp.where(mine, spot, -1), slot, places)
            count = count + mine.astype(jnp.int32)
        return places

    line[...] = lax.fori_loop(0, n, settle_places, jnp.zeros((1, 128), jnp.int32))
    fetch_place = pltpu.make_async_copy(line, place, table_sem.at[3])
    fetch_place.start()

    @pl.when(has_fine)
    def _():
        for k in range(n):
            coarse_arrival(k).wait_recv()
        fetch_fine = pltpu.make_async_copy(fine_tabs, fine_local, table_sem.at[4])
        fetch_fine.start()
        fetch_fine.wait()

    empty = CAP * n

    def settle_octants(source, codes):
        count = jnp.int32(0)
        for b in range(blocks):
            home, spot = split(fine_local[source, 0, b], blocks)
            owner, code = split(fine_local[home, 0, blocks + spot], 8 * blocks)
            mine = owner == me
            hit = jnp.logical_and(mine, fine_local[home, 0, 2 * blocks + spot] == 1)
            slot = CAP * source + jnp.minimum(count, CAP - 1)
            codes = jnp.where(lane == jnp.where(hit, code, -1), slot, codes)
            count = count + mine.astype(jnp.int32)
        return codes

    rounds = jnp.where(has_fine, n, 0)
    line2[...] = lax.fori_loop(0, rounds, settle_octants, jnp.full((1, 128), empty, jnp.int32))
    fetch_octants = pltpu.make_async_copy(line2, octants, table_sem.at[5])
    fetch_octants.start()
    got_ghost[empty] = jnp.zeros(got_ghost.shape[1:], jnp.bfloat16)
    fetch_place.wait()
    fetch_octants.wait()

    wide_lane = lax.broadcasted_iota(jnp.int32, (blocks, 128), 1)
    deep = lax.bitwise_and(wide_lane, 16) != 0
    for corner in range(4):
        mask = jnp.zeros((blocks, 128), jnp.int32)
        for q in range(blocks):
            near_half = (octants[0, q * 8 + corner * 2] < empty).astype(jnp.int32)
            far_half = (octants[0, q * 8 + corner * 2 + 1] < empty).astype(jnp.int32)
            mask = jnp.where(sublane == q, jnp.where(deep, far_half, near_half), mask)
        masks[corner] = mask

    def scatter(part):
        for k in range(1, n):
            block_arrival(part, k).wait_recv()

        def one(q, carry):
            block = gots[part][place[0, q]].astype(jnp.float32)
            for c in range(3):
                at = c * spread + part * piece * blocks + q
                rows[pl.ds(at, piece, stride=blocks), :] = block[c * piece:(c + 1) * piece, :]
            return carry

        lax.fori_loop(0, blocks, one, 0)

    def out_copy(part):
        span = pl.ds(part * SPAN * PLANE, SPAN * PLANE)
        return pltpu.make_async_copy(result.at[:, :, span], out.at[:, :, span], out_sem.at[part])

    def finish(part):
        flagged = [masks[(part * SPAN // 16) * 2 + oy] != 0 for oy in range(2)]

        def one(i, carry):
            x = part * SPAN + i
            for c in range(3):
                for j in range(LANE_TILES):
                    at = c * spread + (x * LANE_TILES + j) * blocks
                    spot = pl.ds(pl.multiple_of(at, blocks), blocks)
                    value = jnp.where(flagged[j // 4], patch[spot, :], rows[spot, :])
                    to = pl.multiple_of(x * PLANE + j * 128, 128)
                    result[c, :, pl.ds(to, 128)] = value.astype(jnp.bfloat16)
            return carry

        lax.fori_loop(0, SPAN, one, 0)
        out_copy(part).start()

    scatter(ORDER[0])
    scatter(ORDER[1])

    @pl.when(has_fine)
    def _():
        for k in range(n):
            ghost_arrival(k).wait_recv()

        def expand(i, carry):
            q, corner = split(i, 4)
            ox, oy = split(corner, 2)
            at = q * 8 + corner * 2
            pair = jnp.concatenate([got_ghost[octants[0, at]], got_ghost[octants[0, at + 1]]], axis=1)
            full = jnp.dot(pair, grow[...], preferred_element_type=jnp.float32)
            for c in range(3):
                for jj in range(4):
                    for half in range(2):
                        x, j = ox * 16 + half * 8, oy * 4 + jj
                        to = c * spread + (x * LANE_TILES + j) * blocks + q
                        patch[pl.ds(to, 8, stride=LANE_TILES * blocks), :] = full[
                            (c * 4 + jj) * 8:(c * 4 + jj + 1) * 8, half * 128:(half + 1) * 128
                        ]
            return carry

        lax.fori_loop(0, 4 * blocks, expand, 0)

    finish(ORDER[0])
    finish(ORDER[1])
    for part in ORDER[2:]:
        scatter(part)
        finish(part)

    @pl.when(not_last)
    def _():
        high(after).wait_send()

    @pl.when(not_first)
    def _():
        low(before).wait_send()

    for k in range(1, n):
        near(k).wait_send()
        for part in ORDER:
            block_copy(part, k).wait_send()

    @pl.when(has_coarse)
    def _():
        for k in range(n):
            coarse(k).wait_send()
            ghost_copy(k).wait_send()

    for part in ORDER:
        out_copy(part).wait()


def selection_tables():
    k = np.arange(1024)
    half, dx, odd, y, z = k // 512, k // 256 % 2, k // 128 % 2, k % 128 // 32, k % 32
    target = half * 64 + (2 * odd + y // 2) * 16 + z // 2
    shrink = np.where(target[:, None] == np.arange(128)[None, :], 0.125, 0.0)
    k = np.arange(256)
    oz, half, y, z = k // 128, k % 128 // 64, k % 64 // 16, k % 16
    target = half * 128 + y * 32 + oz * 16 + z
    grow = np.where(target[:, None] == np.arange(256)[None, :], 1.0, 0.0)
    return shrink, grow


def body(n, levels, vorticity, shift_field, new_index, parent_slot, flags):
    blocks, cells = vorticity.shape[2:]
    vort, shift = vorticity[0], shift_field[0]
    any_space = pl.BlockSpec(memory_space=pl.ANY)
    bf16, f32, i32 = jnp.bfloat16, jnp.float32, jnp.int32
    dma, vm, smem = pltpu.SemaphoreType.DMA, pltpu.VMEM, pltpu.SMEM
    spread = EDGE * LANE_TILES * blocks
    piece = 3 * SPAN * LANE_TILES
    parts = EDGE // SPAN
    shrink, grow = selection_tables()
    out = pl.pallas_call(
        functools.partial(kernel, n, levels),
        out_shape=jax.ShapeDtypeStruct((3, blocks, cells), bf16),
        in_specs=[any_space] * 7,
        out_specs=any_space,
        scratch_shapes=[
            smem((1, blocks), i32), smem((1, blocks), i32), smem((1, blocks), i32),
            vm((4, blocks, cells), bf16), vm(shrink.shape, bf16), vm(grow.shape, bf16),
            vm((3 * spread, 128), f32), vm((3 * spread, 128), f32),
            vm((parts, blocks, piece, 128), bf16), vm((4, blocks, 128), i32), vm((3, blocks, cells), bf16),
            *[vm((n, CAP, piece, 128), bf16)] * parts,
            *[vm((n * CAP, piece, 128), bf16)] * parts,
            vm((blocks, 96, 128), bf16), vm((n, CAP, 96, 128), bf16), vm((n * CAP + 1, 96, 128), bf16),
            vm((128, 128), f32), vm((64, 128), bf16), vm((64, 128), bf16),
            vm((64, 128), bf16), vm((64, 128), bf16), vm((64, 128), f32), vm((64, 128), f32),
            vm((1, 128), i32), vm((n, 1, 128), i32), vm((n, 1, 128), i32),
            smem((n, 1, 128), i32), smem((n, 1, 128), i32),
            vm((1, 128), i32), smem((1, 128), i32), vm((1, 128), i32), smem((1, 128), i32),
            smem((CAP * n,), i32), smem((CAP * n,), i32),
            dma((6,)), dma((3,)), dma((6,)), dma((2,)), dma((2,)), dma((n,)), dma((n,)), dma((n,)), dma((n,)),
            dma((parts, n)), dma((parts, n)), dma((n,)), dma((n,)), dma((parts,)),
            pltpu.SemaphoreType.REGULAR,
        ],
        compiler_params=pltpu.CompilerParams(
            collective_id=0, has_side_effects=True, vmem_limit_bytes=VMEM_LIMIT
        ),
        name="move",
    )(new_index, parent_slot, flags, vort, shift, jnp.asarray(shrink, bf16), jnp.asarray(grow, bf16))
    return out[None]


def solution(mesh):
    placed = (
        P("lvl", None, "blk", None),
        P("lvl", "blk", None),
        P("lvl", "blk"),
        P("lvl", "blk"),
        P("lvl", "blk"),
    )
    step = functools.partial(body, mesh.shape["blk"], mesh.shape["lvl"])
    return jax.shard_map(
        step, mesh=mesh, in_specs=placed, out_specs=P("lvl", None, "blk", None), check_vma=False
    )
```

```python
import functools

import jax
import jax.numpy as jnp
import numpy as np
from jax import lax
from jax.experimental import pallas as pl
from jax.experimental.pallas import tpu as pltpu
from jax.sharding import PartitionSpec as P

MESH = pl.DeviceIdType.MESH
EDGE = 32
PLANE = EDGE * EDGE
LANE_TILES = PLANE // 128
CAP = 2
SPAN = 8
ORDER = (1, 2, 0, 3)
VMEM_LIMIT = 44 * 1024 * 1024
PIECES = ((4 * PLANE, 20 * PLANE), (20 * PLANE, 32 * PLANE), (0, 4 * PLANE))


def device(blk, lvl):
    return {"blk": blk, "lvl": lvl}


def remote(src, dst, send, recv, target):
    return pltpu.make_async_remote_copy(
        src_ref=src, dst_ref=dst, send_sem=send, recv_sem=recv, device_id=target, device_id_type=MESH
    )


def tap_weights(shifts):
    size = jnp.abs(shifts)
    rest = 1.0 - size
    size2 = size * size
    rest2 = rest * rest
    middle = 1.0 + size2 * (1.5 * size - 2.5)
    ahead = 1.0 + rest2 * (1.5 * rest - 2.5)
    behind = -0.5 * rest2 * size
    far = -0.5 * size2 * rest
    up = shifts >= 0.0
    return {
        -2: jnp.where(up, 0.0, far),
        -1: jnp.where(up, behind, ahead),
        0: middle,
        1: jnp.where(up, ahead, behind),
        2: jnp.where(up, far, 0.0),
    }


def split(value, size):
    if size & (size - 1) == 0:
        return lax.shift_right_logical(value, size.bit_length() - 1), lax.bitwise_and(value, size - 1)
    return lax.div(value, size), lax.rem(value, size)


def picks(keys, wanted):
    count, first, second = jnp.int32(0), jnp.int32(0), jnp.int32(0)
    for b, key in enumerate(keys):
        hit = key == wanted
        first = jnp.where(jnp.logical_and(hit, count == 0), b, first)
        second = jnp.where(jnp.logical_and(hit, count == 1), b, second)
        count = count + hit.astype(jnp.int32)
    return first, second


def kernel(n, levels, spots_in, parents_in, flags_in, vort_in, shift_in, shrink_in, grow_in, out,
           spots, parent_slot, flags, field, shrink, grow,
           rows, patch, whole, masks,
           send0, send1, send2, send3, got0, got1, got2, got3,
           small, ghost, relay, got_ghost,
           edge, edge_low, edge_high, below, above, halo_low, halo_high,
           tab, near_tabs, fine_tabs, near_local, fine_local, line, place, line2, octants,
           pick, pick_ghost,
           in_sem, index_sem, table_sem, halo_s, halo_r, near_s, near_r, down_s, down_r,
           block_s, block_r, ghost_s, ghost_r, relay_s, relay_r):
    me = lax.axis_index("blk")
    lvl = lax.axis_index("lvl")
    blocks = out.shape[1]
    spread = EDGE * LANE_TILES * blocks
    piece = SPAN * LANE_TILES
    coarse_level = jnp.maximum(lvl - 1, 0)
    fine_level = jnp.minimum(lvl + 1, levels - 1)
    sends, gots = (send0, send1, send2, send3), (got0, got1, got2, got3)
    after = device(lax.rem(me + 1, n), lvl)
    before = device(lax.rem(me + n - 1, n), lvl)
    below_level = device(me, coarse_level)
    has_coarse, has_fine = lvl > 0, lvl < levels - 1
    not_first, not_last = me > 0, me < n - 1

    barrier = pltpu.get_barrier_semaphore()

    def greet(blk, level):
        pl.semaphore_signal(barrier, inc=1, device_id=device(blk, level), device_id_type=MESH)

    for k in range(1, n):
        greet(lax.rem(me + k, n), lvl)

    @pl.when(has_coarse)
    def _():
        greet(me, coarse_level)

    @pl.when(has_fine)
    def _():
        greet(me, fine_level)

    index_loads = [
        pltpu.make_async_copy(src, dst, index_sem.at[i])
        for i, (src, dst) in enumerate(((spots_in, spots), (parents_in, parent_slot), (flags_in, flags)))
    ]
    loads = []
    for i, (lo, hi) in enumerate(PIECES):
        part = pl.ds(lo, hi - lo)
        loads.append((
            pltpu.make_async_copy(shift_in.at[:, part], field.at[3, :, part], in_sem.at[2 * i]),
            pltpu.make_async_copy(vort_in.at[:, :, part], field.at[pl.ds(0, 3), :, part], in_sem.at[2 * i + 1]),
        ))
    constants = (
        pltpu.make_async_copy(shrink_in, shrink, table_sem.at[0]),
        pltpu.make_async_copy(grow_in, grow, table_sem.at[1]),
    )
    for copy in index_loads:
        copy.start()
    for pair in loads:
        for copy in pair:
            copy.start()
    for copy in constants:
        copy.start()

    sublane = lax.broadcasted_iota(jnp.int32, (blocks, 128), 0)
    lane = lax.broadcasted_iota(jnp.int32, (1, 128), 1)

    def tile(f, x, j):
        at = pl.multiple_of(x * PLANE + j * 128, 128)
        return field[f, :, pl.ds(at, 128)].astype(jnp.float32)

    def source_tile(f, x, j):
        if x < 0:
            edge_row = halo_low[pl.ds(f * 16 + (x + 2) * LANE_TILES + j, 1), :]
            return jnp.where(sublane == 0, edge_row, pltpu.roll(tile(f, x + EDGE, j), 1, 0))
        if x >= EDGE:
            edge_row = halo_high[pl.ds(f * 16 + (x - EDGE) * LANE_TILES + j, 1), :]
            return jnp.where(sublane == blocks - 1, edge_row, pltpu.roll(tile(f, x - EDGE, j), blocks - 1, 0))
        return tile(f, x, j)

    def remesh(part):
        x0, x1 = part * SPAN, (part + 1) * SPAN

        def chunk(j, carry):
            sums = [{}, {}, {}]
            for x in range(x0 - 2, x1 + 2):
                weights = tap_weights(source_tile(3, x, j))
                for c in range(3):
                    value = source_tile(c, x, j)
                    for offset in range(-2, 3):
                        to = x + offset
                        if x0 <= to < x1:
                            term = value * weights[offset]
                            sums[c][to] = sums[c][to] + term if to in sums[c] else term
                    if x0 <= x - 2:
                        at = c * spread + ((x - 2) * LANE_TILES + j) * blocks
                        rows[pl.ds(pl.multiple_of(at, blocks), blocks), :] = sums[c].pop(x - 2)
            return carry

        lax.fori_loop(0, LANE_TILES, chunk, 0)
        for b in range(blocks):
            for c in range(3):
                at = c * spread + x0 * LANE_TILES * blocks + b
                whole[part, b, c * piece:(c + 1) * piece, :] = rows[
                    pl.ds(at, piece, stride=blocks), :
                ].astype(jnp.bfloat16)

    def pack(part):
        def one(k, carry):
            to = lax.rem(me + k, n)
            for s in range(CAP):
                sends[part][to, s] = whole[part, pick[CAP * to + s]]
            return carry

        lax.fori_loop(1, n, one, 0)

    def keep(part):
        for s in range(CAP):
            gots[part][CAP * me + s] = whole[part, pick[CAP * me + s]]

    def block_copy(part, k):
        to = lax.rem(me + k, n)
        return remote(sends[part].at[to], gots[part].at[pl.ds(CAP * me, CAP)],
                      block_s.at[part, k], block_r.at[part, k], device(to, lvl))

    def block_arrival(part, k):
        source = lax.rem(me + n - k, n)
        return remote(sends[part].at[me], gots[part].at[pl.ds(CAP * source, CAP)],
                      block_s.at[part, k], block_r.at[part, k], before)

    def send_blocks(part):
        for k in range(1, n):
            block_copy(part, k).start()

    def near(k):
        return remote(tab, near_tabs.at[me], near_s.at[k], near_r.at[k], device(lax.rem(me + k, n), lvl))

    def near_arrival(k):
        return remote(tab, near_tabs.at[lax.rem(me + n - k, n)], near_s.at[k], near_r.at[k], before)

    def down():
        return remote(near_tabs, fine_tabs, down_s, down_r, below_level)

    def ghost_copy(k):
        to = lax.rem(me + k, n)
        return remote(ghost.at[to], relay.at[pl.ds(CAP * me, CAP)], ghost_s.at[k], ghost_r.at[k], device(to, lvl))

    def ghost_arrival(k):
        source = lax.rem(me + n - k, n)
        return remote(ghost.at[me], relay.at[pl.ds(CAP * source, CAP)], ghost_s.at[k], ghost_r.at[k], before)

    def relay_copy(k):
        source = lax.rem(me + n - k, n)
        pair = pl.ds(CAP * source, CAP)
        origin = ghost.at[me] if k == 0 else relay.at[pair]
        return remote(origin, got_ghost.at[pair], relay_s.at[k], relay_r.at[k], below_level)

    def high(target):
        return remote(edge_high, below, halo_s.at[0], halo_r.at[0], target)

    def low(target):
        return remote(edge_low, above, halo_s.at[1], halo_r.at[1], target)

    for copy in index_loads:
        copy.wait()
    head = jnp.zeros((1, 128), jnp.int32)
    for part, ref in enumerate((spots, parent_slot, flags)):
        for b in range(blocks):
            head = jnp.where(lane == part * blocks + b, ref[0, b], head)
    tab[...] = head
    near_tabs[me] = head
    owners = [split(spots[0, b], blocks)[0] for b in range(blocks)]

    def choose(to, carry):
        first, second = picks(owners, to)
        pick[CAP * to] = first
        pick[CAP * to + 1] = second
        return carry

    lax.fori_loop(0, n, choose, 0)

    for copy in loads[0]:
        copy.wait()
    remesh(ORDER[0])
    pack(ORDER[0])
    for copy in loads[1] + loads[2]:
        copy.wait()

    def edges(j, carry):
        for f in range(4):
            for p in range(2):
                at = f * 16 + p * LANE_TILES + j
                edge[pl.ds(at, 1), :] = tile(f, p, j)[0:1, :]
                edge[pl.ds(64 + at, 1), :] = tile(f, EDGE - 2 + p, j)[blocks - 1:blocks, :]
        return carry

    lax.fori_loop(0, LANE_TILES, edges, 0)
    edge_low[...] = edge[0:64, :].astype(jnp.bfloat16)
    edge_high[...] = edge[64:128, :].astype(jnp.bfloat16)

    nearby = n - 1 + has_coarse.astype(jnp.int32) + has_fine.astype(jnp.int32)
    pl.semaphore_wait(barrier, nearby)

    @pl.when(not_last)
    def _():
        high(after).start()

    @pl.when(not_first)
    def _():
        low(before).start()

    for k in range(1, n):
        near(k).start()
    send_blocks(ORDER[0])

    keep(ORDER[0])
    remesh(ORDER[1])
    pack(ORDER[1])
    send_blocks(ORDER[1])
    keep(ORDER[1])

    @pl.when(not_last)
    def _():
        low(after).wait_recv()

    @pl.when(not_first)
    def _():
        high(before).wait_recv()

    halo_low[...] = jnp.where(not_first, below[...].astype(jnp.float32), 0.0)
    halo_high[...] = jnp.where(not_last, above[...].astype(jnp.float32), 0.0)
    for part in ORDER[2:]:
        remesh(part)
        pack(part)
        keep(part)

    for k in range(1, n):
        near_arrival(k).wait_recv()

    @pl.when(has_coarse)
    def _():
        down().start()

    fetch_near = pltpu.make_async_copy(near_tabs, near_local, table_sem.at[2])
    fetch_near.start()
    fetch_near.wait()
    for copy in constants:
        copy.wait()

    @pl.when(has_coarse)
    def _():
        parents = []
        for b in range(blocks):
            home, spot = split(spots[0, b], blocks)
            parents.append(split(near_local[home, 0, blocks + spot], 8 * blocks)[0])

        def choose_ghost(to, carry):
            first, second = picks(parents, to)
            pick_ghost[CAP * to] = first
            pick_ghost[CAP * to + 1] = second
            return carry

        lax.fori_loop(0, n, choose_ghost, 0)

        def restrict(b, carry):
            columns = []
            for half in range(2):
                for dx in range(2):
                    for odd in range(2):
                        parts = []
                        for c in range(3):
                            for jj in range(4):
                                x, j = half * 16 + dx, 2 * jj + odd
                                at = c * spread + (x * LANE_TILES + j) * blocks + b
                                parts.append(rows[pl.ds(at, 8, stride=2 * LANE_TILES * blocks), :])
                        columns.append(jnp.concatenate(parts, axis=0).astype(jnp.bfloat16))
            wide = jnp.concatenate(columns, axis=1)
            small[b] = jnp.dot(wide, shrink[...], preferred_element_type=jnp.float32).astype(jnp.bfloat16)
            return carry

        lax.fori_loop(0, blocks, restrict, 0)

        def pack_ghost(to, carry):
            for s in range(CAP):
                ghost[to, s] = small[pick_ghost[CAP * to + s]]
            return carry

        lax.fori_loop(0, n, pack_ghost, 0)
        for k in range(1, n):
            ghost_copy(k).start()
        relay_copy(0).start()

    for part in ORDER[2:]:
        send_blocks(part)

    def settle_places(source, places):
        count = jnp.int32(0)
        for b in range(blocks):
            owner, spot = split(near_local[source, 0, b], blocks)
            mine = owner == me
            slot = CAP * source + jnp.minimum(count, CAP - 1)
            places = jnp.where(lane == jnp.where(mine, spot, -1), slot, places)
            count = count + mine.astype(jnp.int32)
        return places

    line[...] = lax.fori_loop(0, n, settle_places, jnp.zeros((1, 128), jnp.int32))
    fetch_place = pltpu.make_async_copy(line, place, table_sem.at[3])
    fetch_place.start()

    @pl.when(has_fine)
    def _():
        down().wait_recv()
        fetch_fine = pltpu.make_async_copy(fine_tabs, fine_local, table_sem.at[4])
        fetch_fine.start()
        fetch_fine.wait()

    empty = CAP * n

    def settle_octants(source, codes):
        count = jnp.int32(0)
        for b in range(blocks):
            home, spot = split(fine_local[source, 0, b], blocks)
            owner, code = split(fine_local[home, 0, blocks + spot], 8 * blocks)
            mine = owner == me
            hit = jnp.logical_and(mine, fine_local[home, 0, 2 * blocks + spot] == 1)
            slot = CAP * source + jnp.minimum(count, CAP - 1)
            codes = jnp.where(lane == jnp.where(hit, code, -1), slot, codes)
            count = count + mine.astype(jnp.int32)
        return codes

    rounds = jnp.where(has_fine, n, 0)
    line2[...] = lax.fori_loop(0, rounds, settle_octants, jnp.full((1, 128), empty, jnp.int32))
    fetch_octants = pltpu.make_async_copy(line2, octants, table_sem.at[5])
    fetch_octants.start()
    got_ghost[empty] = jnp.zeros(got_ghost.shape[1:], jnp.bfloat16)
    fetch_place.wait()
    fetch_octants.wait()

    wide_lane = lax.broadcasted_iota(jnp.int32, (blocks, 128), 1)
    deep = lax.bitwise_and(wide_lane, 16) != 0
    for corner in range(4):
        mask = jnp.zeros((blocks, 128), jnp.int32)
        for q in range(blocks):
            near_half = (octants[0, q * 8 + corner * 2] < empty).astype(jnp.int32)
            far_half = (octants[0, q * 8 + corner * 2 + 1] < empty).astype(jnp.int32)
            mask = jnp.where(sublane == q, jnp.where(deep, far_half, near_half), mask)
        masks[corner] = mask

    def scatter(part):
        for k in range(1, n):
            block_arrival(part, k).wait_recv()

        def one(q, carry):
            block = gots[part][place[0, q]].astype(jnp.float32)
            for c in range(3):
                at = c * spread + part * piece * blocks + q
                rows[pl.ds(at, piece, stride=blocks), :] = block[c * piece:(c + 1) * piece, :]
            return carry

        lax.fori_loop(0, blocks, one, 0)

    def finish(part):
        flagged = [masks[(part * SPAN // 16) * 2 + oy] != 0 for oy in range(2)]

        def one(i, carry):
            x = part * SPAN + i
            for c in range(3):
                for j in range(LANE_TILES):
                    at = c * spread + (x * LANE_TILES + j) * blocks
                    spot = pl.ds(pl.multiple_of(at, blocks), blocks)
                    value = jnp.where(flagged[j // 4], patch[spot, :], rows[spot, :])
                    to = pl.multiple_of(x * PLANE + j * 128, 128)
                    out[c, :, pl.ds(to, 128)] = value.astype(jnp.bfloat16)
            return carry

        lax.fori_loop(0, SPAN, one, 0)

    scatter(ORDER[0])
    scatter(ORDER[1])

    @pl.when(has_coarse)
    def _():
        for k in range(1, n):
            ghost_arrival(k).wait_recv()
            relay_copy(k).start()

    scatter(ORDER[2])

    @pl.when(has_fine)
    def _():
        for k in range(n):
            relay_copy(k).wait_recv()

        def expand(i, carry):
            q, corner = split(i, 4)
            ox, oy = split(corner, 2)
            at = q * 8 + corner * 2
            pair = jnp.concatenate([got_ghost[octants[0, at]], got_ghost[octants[0, at + 1]]], axis=1)
            full = jnp.dot(pair, grow[...], preferred_element_type=jnp.float32)
            for c in range(3):
                for jj in range(4):
                    for half in range(2):
                        x, j = ox * 16 + half * 8, oy * 4 + jj
                        to = c * spread + (x * LANE_TILES + j) * blocks + q
                        patch[pl.ds(to, 8, stride=LANE_TILES * blocks), :] = full[
                            (c * 4 + jj) * 8:(c * 4 + jj + 1) * 8, half * 128:(half + 1) * 128
                        ]
            return carry

        lax.fori_loop(0, 4 * blocks, expand, 0)

    for part in ORDER[:3]:
        finish(part)
    scatter(ORDER[3])
    finish(ORDER[3])

    @pl.when(not_last)
    def _():
        high(after).wait_send()

    @pl.when(not_first)
    def _():
        low(before).wait_send()

    for k in range(1, n):
        near(k).wait_send()
        for part in ORDER:
            block_copy(part, k).wait_send()

    @pl.when(has_coarse)
    def _():
        down().wait_send()
        for k in range(1, n):
            ghost_copy(k).wait_send()
        for k in range(n):
            relay_copy(k).wait_send()


def selection_tables():
    k = np.arange(1024)
    half, dx, odd, y, z = k // 512, k // 256 % 2, k // 128 % 2, k % 128 // 32, k % 32
    target = half * 64 + (2 * odd + y // 2) * 16 + z // 2
    shrink = np.where(target[:, None] == np.arange(128)[None, :], 0.125, 0.0)
    k = np.arange(256)
    oz, half, y, z = k // 128, k % 128 // 64, k % 64 // 16, k % 16
    target = half * 128 + y * 32 + oz * 16 + z
    grow = np.where(target[:, None] == np.arange(256)[None, :], 1.0, 0.0)
    return shrink, grow


def body(n, levels, vorticity, shift_field, new_index, parent_slot, flags):
    blocks, cells = vorticity.shape[2:]
    vort, shift = vorticity[0], shift_field[0]
    hbm = pl.BlockSpec(memory_space=pltpu.HBM)
    vmem = pl.BlockSpec(memory_space=pltpu.VMEM)
    bf16, f32, i32 = jnp.bfloat16, jnp.float32, jnp.int32
    dma, vm, smem = pltpu.SemaphoreType.DMA, pltpu.VMEM, pltpu.SMEM
    spread = EDGE * LANE_TILES * blocks
    piece = 3 * SPAN * LANE_TILES
    parts = EDGE // SPAN
    shrink, grow = selection_tables()
    out = pl.pallas_call(
        functools.partial(kernel, n, levels),
        out_shape=jax.ShapeDtypeStruct((3, blocks, cells), bf16),
        in_specs=[hbm] * 7,
        out_specs=vmem,
        scratch_shapes=[
            smem((1, blocks), i32), smem((1, blocks), i32), smem((1, blocks), i32),
            vm((4, blocks, cells), bf16), vm(shrink.shape, bf16), vm(grow.shape, bf16),
            vm((3 * spread, 128), f32), vm((3 * spread, 128), f32),
            vm((parts, blocks, piece, 128), bf16), vm((4, blocks, 128), i32),
            *[vm((n, CAP, piece, 128), bf16)] * parts,
            *[vm((n * CAP, piece, 128), bf16)] * parts,
            vm((blocks, 96, 128), bf16), vm((n, CAP, 96, 128), bf16), vm((n * CAP, 96, 128), bf16),
            vm((n * CAP + 1, 96, 128), bf16),
            vm((128, 128), f32), vm((64, 128), bf16), vm((64, 128), bf16),
            vm((64, 128), bf16), vm((64, 128), bf16), vm((64, 128), f32), vm((64, 128), f32),
            vm((1, 128), i32), vm((n, 1, 128), i32), vm((n, 1, 128), i32),
            smem((n, 1, 128), i32), smem((n, 1, 128), i32),
            vm((1, 128), i32), smem((1, 128), i32), vm((1, 128), i32), smem((1, 128), i32),
            smem((CAP * n,), i32), smem((CAP * n,), i32),
            dma((6,)), dma((3,)), dma((6,)), dma((2,)), dma((2,)), dma((n,)), dma((n,)), dma, dma,
            dma((parts, n)), dma((parts, n)), dma((n,)), dma((n,)), dma((n,)), dma((n,)),
        ],
        compiler_params=pltpu.CompilerParams(
            collective_id=0, has_side_effects=True, vmem_limit_bytes=VMEM_LIMIT
        ),
        name="move",
    )(*[
        pltpu.with_memory_space_constraint(x, pltpu.HBM)
        for x in (new_index, parent_slot, flags, vort, shift, jnp.asarray(shrink, bf16), jnp.asarray(grow, bf16))
    ])
    return out[None]


def solution(mesh):
    placed = (
        P("lvl", None, "blk", None),
        P("lvl", "blk", None),
        P("lvl", "blk"),
        P("lvl", "blk"),
        P("lvl", "blk"),
    )
    step = functools.partial(body, mesh.shape["blk"], mesh.shape["lvl"])
    return jax.shard_map(
        step, mesh=mesh, in_specs=placed, out_specs=P("lvl", None, "blk", None), check_vma=False
    )
```

```python
import functools

import jax
import jax.numpy as jnp
import numpy as np
from jax import lax
from jax.experimental import pallas as pl
from jax.experimental.pallas import tpu as pltpu
from jax.sharding import PartitionSpec as P

MESH = pl.DeviceIdType.MESH
EDGE = 32
PLANE = EDGE * EDGE
LANE_TILES = PLANE // 128
CAP = 2
SPAN = 8
ORDER = (1, 2, 0, 3)
VMEM_LIMIT = 44 * 1024 * 1024
PIECES = ((4 * PLANE, 20 * PLANE), (20 * PLANE, 32 * PLANE), (0, 4 * PLANE))


def device(blk, lvl):
    return {"blk": blk, "lvl": lvl}


def remote(src, dst, send, recv, target):
    return pltpu.make_async_remote_copy(
        src_ref=src, dst_ref=dst, send_sem=send, recv_sem=recv, device_id=target, device_id_type=MESH
    )


def tap_weights(shifts):
    size = jnp.abs(shifts)
    rest = 1.0 - size
    size2 = size * size
    rest2 = rest * rest
    middle = 1.0 + size2 * (1.5 * size - 2.5)
    ahead = 1.0 + rest2 * (1.5 * rest - 2.5)
    behind = -0.5 * rest2 * size
    far = -0.5 * size2 * rest
    up = shifts >= 0.0
    return {
        -2: jnp.where(up, 0.0, far),
        -1: jnp.where(up, behind, ahead),
        0: middle,
        1: jnp.where(up, ahead, behind),
        2: jnp.where(up, far, 0.0),
    }


def split(value, size):
    if size & (size - 1) == 0:
        return lax.shift_right_logical(value, size.bit_length() - 1), lax.bitwise_and(value, size - 1)
    return lax.div(value, size), lax.rem(value, size)


def picks(keys, wanted):
    count, first, second = jnp.int32(0), jnp.int32(0), jnp.int32(0)
    for b, key in enumerate(keys):
        hit = key == wanted
        first = jnp.where(jnp.logical_and(hit, count == 0), b, first)
        second = jnp.where(jnp.logical_and(hit, count == 1), b, second)
        count = count + hit.astype(jnp.int32)
    return first, second


def flip(value, mask):
    for bit in range(mask.bit_length()):
        if mask >> bit & 1:
            value = value + (1 << bit) * (1 - 2 * lax.rem(lax.div(value, 1 << bit), 2))
    return value


def groups(n):
    others = range(1, n)
    if n < 8 or n & (n - 1):
        return list(others), [], []
    bits = n.bit_length() - 1
    across = ((1 << (bits - 1) // 2) - 1) << 1
    along = (n - 1) & ~across & ~1
    far = [k for k in others if k & across and k & along]
    close = sorted((k for k in others if k not in far), key=lambda k: (k == 1, k & 1, k))
    return close, far, [k for k in others if k & ~across == 0]


def shared_rows(lvl, levels):
    return 16 * min(max(round(6 * lvl / levels), 1), 5)


def kernel(n, levels, spots_in, parents_in, flags_in, vort_in, shift_in, shrink_in, grow_in, out,
           spots, parent_slot, flags, field, shrink, grow,
           rows, patch, whole, masks,
           send0, send1, send2, send3, got0, got1, got2, got3,
           small, ghost, relay, got_ghost,
           edge, edge_low, edge_high, below, above, halo_low, halo_high,
           tab, near_tabs, fine_tabs, near_local, fine_local, line, place, line2, octants,
           pick, pick_ghost,
           in_sem, index_sem, table_sem, halo_s, halo_r, near_s, near_r, down_s, down_r,
           block_s, block_r, ghost_s, ghost_r, relay_s, relay_r, direct_s, direct_r,
           cross_ready, plane_ready):
    me = lax.axis_index("blk")
    lvl = lax.axis_index("lvl")
    blocks = out.shape[1]
    spread = EDGE * LANE_TILES * blocks
    piece = SPAN * LANE_TILES
    pitch = (LANE_TILES + 1) * blocks
    coarse_level = jnp.maximum(lvl - 1, 0)
    fine_level = jnp.minimum(lvl + 1, levels - 1)
    sends, gots = (send0, send1, send2, send3), (got0, got1, got2, got3)
    after = device(lax.rem(me + 1, n), lvl)
    before = device(lax.rem(me + n - 1, n), lvl)
    below_level = device(me, coarse_level)
    has_coarse, has_fine = lvl > 0, lvl < levels - 1
    not_first, not_last = me > 0, me < n - 1

    close, far, cross = groups(n)
    everyone = close + far
    if n & (n - 1):
        partners = [lax.rem(me + k, n) for k in range(n)]
        sources = [lax.rem(me + n - k, n) for k in range(n)]
    else:
        partners = sources = [flip(me, k) for k in range(n)]

    barrier = pltpu.get_barrier_semaphore()

    def greet(blk, level):
        pl.semaphore_signal(barrier, inc=1, device_id=device(blk, level), device_id_type=MESH)

    for k in close:
        greet(partners[k], lvl)

    @pl.when(has_fine)
    def _():
        greet(me, fine_level)

    index_loads = [
        pltpu.make_async_copy(src, dst, index_sem.at[i])
        for i, (src, dst) in enumerate(((spots_in, spots), (parents_in, parent_slot), (flags_in, flags)))
    ]
    loads = []
    for i, (lo, hi) in enumerate(PIECES):
        part = pl.ds(lo, hi - lo)
        loads.append((
            pltpu.make_async_copy(shift_in.at[:, part], field.at[3, :, part], in_sem.at[2 * i]),
            pltpu.make_async_copy(vort_in.at[:, :, part], field.at[pl.ds(0, 3), :, part], in_sem.at[2 * i + 1]),
        ))
    constants = (
        pltpu.make_async_copy(shrink_in, shrink, table_sem.at[0]),
        pltpu.make_async_copy(grow_in, grow, table_sem.at[1]),
    )
    for copy in index_loads:
        copy.start()
    for pair in loads:
        for copy in pair:
            copy.start()
    for copy in constants:
        copy.start()

    sublane = lax.broadcasted_iota(jnp.int32, (blocks, 128), 0)
    lane = lax.broadcasted_iota(jnp.int32, (1, 128), 1)

    def tile(f, x, j):
        at = pl.multiple_of(x * PLANE + j * 128, 128)
        return field[f, :, pl.ds(at, 128)].astype(jnp.float32)

    def source_tile(f, x, j):
        if x < 0:
            edge_row = halo_low[pl.ds(f * 16 + (x + 2) * LANE_TILES + j, 1), :]
            return jnp.where(sublane == 0, edge_row, pltpu.roll(tile(f, x + EDGE, j), 1, 0))
        if x >= EDGE:
            edge_row = halo_high[pl.ds(f * 16 + (x - EDGE) * LANE_TILES + j, 1), :]
            return jnp.where(sublane == blocks - 1, edge_row, pltpu.roll(tile(f, x - EDGE, j), blocks - 1, 0))
        return tile(f, x, j)

    def remesh(part):
        x0, x1 = part * SPAN, (part + 1) * SPAN

        def chunk(j, carry):
            sums = [{}, {}, {}]
            for x in range(x0 - 2, x1 + 2):
                weights = tap_weights(source_tile(3, x, j))
                for c in range(3):
                    value = source_tile(c, x, j)
                    for offset in range(-2, 3):
                        to = x + offset
                        if x0 <= to < x1:
                            term = value * weights[offset]
                            sums[c][to] = sums[c][to] + term if to in sums[c] else term
                    if x0 <= x - 2:
                        at = c * spread + ((x - 2) * LANE_TILES + j) * blocks
                        rows[pl.ds(pl.multiple_of(at, blocks), blocks), :] = sums[c].pop(x - 2)
            return carry

        lax.fori_loop(0, LANE_TILES, chunk, 0)
        for b in range(blocks):
            for c in range(3):
                at = c * spread + x0 * LANE_TILES * blocks + b
                whole[part, b, c * piece:(c + 1) * piece, :] = rows[
                    pl.ds(at, piece, stride=blocks), :
                ].astype(jnp.bfloat16)

    def pack(part):
        def one(to, carry):
            for s in range(CAP):
                sends[part][to, s] = whole[part, pick[CAP * to + s]]
            return carry

        lax.fori_loop(0, n, one, 0)

    def keep(part):
        for s in range(CAP):
            gots[part][CAP * me + s] = whole[part, pick[CAP * me + s]]

    def block_copy(part, k):
        to = partners[k]
        return remote(sends[part].at[to], gots[part].at[pl.ds(CAP * me, CAP)],
                      block_s.at[part, k], block_r.at[part, k], device(to, lvl))

    def block_arrival(part, k):
        source = sources[k]
        return remote(sends[part].at[me], gots[part].at[pl.ds(CAP * source, CAP)],
                      block_s.at[part, k], block_r.at[part, k], before)

    def send_blocks(part, group):
        for k in group:
            block_copy(part, k).start()

    def near(k):
        return remote(tab, near_tabs.at[me], near_s.at[k], near_r.at[k], device(partners[k], lvl))

    def near_arrival(k):
        return remote(tab, near_tabs.at[sources[k]], near_s.at[k], near_r.at[k], before)

    def down():
        return remote(near_tabs, fine_tabs, down_s, down_r, below_level)

    def ghost_copy(k, size):
        part = pl.ds(0, size)
        return remote(ghost.at[partners[k], :, part], relay.at[pl.ds(CAP * me, CAP), part],
                      ghost_s.at[k], ghost_r.at[k], device(partners[k], lvl))

    def ghost_arrival(k, size):
        part = pl.ds(0, size)
        return remote(ghost.at[me, :, part], relay.at[pl.ds(CAP * sources[k], CAP), part],
                      ghost_s.at[k], ghost_r.at[k], before)

    def relay_copy(k, size):
        pair, part = pl.ds(CAP * sources[k], CAP), pl.ds(0, size)
        origin = ghost.at[me, :, part] if k == 0 else relay.at[pair, part]
        return remote(origin, got_ghost.at[pair, part], relay_s.at[k], relay_r.at[k], below_level)

    def direct_copy(k, size):
        part = pl.ds(size, 96 - size)
        return remote(ghost.at[partners[k], :, part], got_ghost.at[pl.ds(CAP * me, CAP), part],
                      direct_s.at[k], direct_r.at[k], device(partners[k], coarse_level))

    def direct_arrival(k, size):
        part = pl.ds(size, 96 - size)
        return remote(ghost.at[me, :, part], got_ghost.at[pl.ds(CAP * sources[k], CAP), part],
                      direct_s.at[k], direct_r.at[k], before)

    def on_level(shift, action):
        for level in range(1, levels):
            pl.when(lvl == level - shift)(functools.partial(action, shared_rows(level, levels)))

    def high(target):
        return remote(edge_high, below, halo_s.at[0], halo_r.at[0], target)

    def low(target):
        return remote(edge_low, above, halo_s.at[1], halo_r.at[1], target)

    for copy in index_loads:
        copy.wait()
    head = jnp.zeros((1, 128), jnp.int32)
    for part, ref in enumerate((spots, parent_slot, flags)):
        for b in range(blocks):
            head = jnp.where(lane == part * blocks + b, ref[0, b], head)
    tab[...] = head
    near_tabs[me] = head
    owners = [split(spots[0, b], blocks)[0] for b in range(blocks)]

    def choose(to, carry):
        first, second = picks(owners, to)
        pick[CAP * to] = first
        pick[CAP * to + 1] = second
        return carry

    lax.fori_loop(0, n, choose, 0)

    for copy in loads[0]:
        copy.wait()
    remesh(ORDER[0])
    pack(ORDER[0])
    for copy in loads[1] + loads[2]:
        copy.wait()

    def edges(j, carry):
        for f in range(4):
            for p in range(2):
                at = f * 16 + p * LANE_TILES + j
                edge[pl.ds(at, 1), :] = tile(f, p, j)[0:1, :]
                edge[pl.ds(64 + at, 1), :] = tile(f, EDGE - 2 + p, j)[blocks - 1:blocks, :]
        return carry

    lax.fori_loop(0, LANE_TILES, edges, 0)
    edge_low[...] = edge[0:64, :].astype(jnp.bfloat16)
    edge_high[...] = edge[64:128, :].astype(jnp.bfloat16)

    pl.semaphore_wait(barrier, len(close) + has_coarse.astype(jnp.int32))
    for k in cross:
        pl.semaphore_signal(cross_ready, inc=1, device_id=device(partners[k], lvl), device_id_type=MESH)
    for k in close:
        near(k).start()
    send_blocks(ORDER[0], close)
    if cross:
        pl.semaphore_wait(cross_ready, len(cross))

    @pl.when(not_last)
    def _():
        high(after).start()

    @pl.when(not_first)
    def _():
        low(before).start()

    for k in far:
        near(k).start()
    send_blocks(ORDER[0], far)
    keep(ORDER[0])
    remesh(ORDER[1])
    pack(ORDER[1])
    send_blocks(ORDER[1], everyone)
    keep(ORDER[1])

    @pl.when(not_last)
    def _():
        low(after).wait_recv()

    @pl.when(not_first)
    def _():
        high(before).wait_recv()

    halo_low[...] = jnp.where(not_first, below[...].astype(jnp.float32), 0.0)
    halo_high[...] = jnp.where(not_last, above[...].astype(jnp.float32), 0.0)
    for part in ORDER[2:]:
        remesh(part)
        pack(part)
        keep(part)

    for k in range(1, n):
        near_arrival(k).wait_recv()

    @pl.when(has_coarse)
    def _():
        down().start()

    fetch_near = pltpu.make_async_copy(near_tabs, near_local, table_sem.at[2])
    fetch_near.start()
    fetch_near.wait()
    for copy in constants:
        copy.wait()

    @pl.when(has_coarse)
    def _():
        parents = []
        for b in range(blocks):
            home, spot = split(spots[0, b], blocks)
            parents.append(split(near_local[home, 0, blocks + spot], 8 * blocks)[0])

        def choose_ghost(to, carry):
            first, second = picks(parents, to)
            pick_ghost[CAP * to] = first
            pick_ghost[CAP * to + 1] = second
            return carry

        lax.fori_loop(0, n, choose_ghost, 0)

        def restrict(b, carry):
            columns = []
            for half in range(2):
                for dx in range(2):
                    for odd in range(2):
                        parts = []
                        for c in range(3):
                            for jj in range(4):
                                x, j = half * 16 + dx, 2 * jj + odd
                                at = c * spread + (x * LANE_TILES + j) * blocks + b
                                parts.append(rows[pl.ds(at, 8, stride=2 * LANE_TILES * blocks), :])
                        columns.append(jnp.concatenate(parts, axis=0).astype(jnp.bfloat16))
            wide = jnp.concatenate(columns, axis=1)
            small[b] = jnp.dot(wide, shrink[...], preferred_element_type=jnp.float32).astype(jnp.bfloat16)
            return carry

        lax.fori_loop(0, blocks, restrict, 0)

        def pack_ghost(to, carry):
            for s in range(CAP):
                ghost[to, s] = small[pick_ghost[CAP * to + s]]
            return carry

        lax.fori_loop(0, n, pack_ghost, 0)

    def share(size):
        for k in everyone:
            ghost_copy(k, size).start()
        relay_copy(0, size).start()

    on_level(0, share)
    for part in ORDER[2:]:
        send_blocks(part, everyone)

    def settle_places(source, places):
        count = jnp.int32(0)
        for b in range(blocks):
            owner, spot = split(near_local[source, 0, b], blocks)
            mine = owner == me
            slot = CAP * source + jnp.minimum(count, CAP - 1)
            places = jnp.where(lane == jnp.where(mine, spot, -1), slot, places)
            count = count + mine.astype(jnp.int32)
        return places

    line[...] = lax.fori_loop(0, n, settle_places, jnp.zeros((1, 128), jnp.int32))
    fetch_place = pltpu.make_async_copy(line, place, table_sem.at[3])
    fetch_place.start()

    @pl.when(has_fine)
    def _():
        down().wait_recv()
        pl.semaphore_signal(plane_ready, inc=1, device_id=device(me, fine_level), device_id_type=MESH)
        fetch_fine = pltpu.make_async_copy(fine_tabs, fine_local, table_sem.at[4])
        fetch_fine.start()
        fetch_fine.wait()

    @pl.when(has_coarse)
    def _():
        pl.semaphore_wait(plane_ready, 1)

    def rest(size):
        for k in [0] + everyone:
            direct_copy(k, size).start()

    on_level(0, rest)
    empty = CAP * n

    def settle_octants(source, codes):
        count = jnp.int32(0)
        for b in range(blocks):
            home, spot = split(fine_local[source, 0, b], blocks)
            owner, code = split(fine_local[home, 0, blocks + spot], 8 * blocks)
            mine = owner == me
            hit = jnp.logical_and(mine, fine_local[home, 0, 2 * blocks + spot] == 1)
            slot = CAP * source + jnp.minimum(count, CAP - 1)
            codes = jnp.where(lane == jnp.where(hit, code, -1), slot, codes)
            count = count + mine.astype(jnp.int32)
        return codes

    rounds = jnp.where(has_fine, n, 0)
    line2[...] = lax.fori_loop(0, rounds, settle_octants, jnp.full((1, 128), empty, jnp.int32))
    fetch_octants = pltpu.make_async_copy(line2, octants, table_sem.at[5])
    fetch_octants.start()
    got_ghost[empty] = jnp.zeros(got_ghost.shape[1:], jnp.bfloat16)
    fetch_place.wait()
    fetch_octants.wait()

    wide_lane = lax.broadcasted_iota(jnp.int32, (blocks, 128), 1)
    deep = lax.bitwise_and(wide_lane, 16) != 0
    for corner in range(4):
        mask = jnp.zeros((blocks, 128), jnp.int32)
        for q in range(blocks):
            near_half = (octants[0, q * 8 + corner * 2] < empty).astype(jnp.int32)
            far_half = (octants[0, q * 8 + corner * 2 + 1] < empty).astype(jnp.int32)
            mask = jnp.where(sublane == q, jnp.where(deep, far_half, near_half), mask)
        masks[corner] = mask

    def scatter(part):
        for k in range(1, n):
            block_arrival(part, k).wait_recv()

        def one(q, carry):
            block = gots[part][place[0, q]].astype(jnp.float32)
            for c in range(3):
                at = c * spread + part * piece * blocks + q
                rows[pl.ds(at, piece, stride=blocks), :] = block[c * piece:(c + 1) * piece, :]
            return carry

        lax.fori_loop(0, blocks, one, 0)

    def finish(part):
        flagged = [masks[(part * SPAN // 16) * 2 + oy] != 0 for oy in range(2)]

        def one(i, carry):
            x = part * SPAN + i
            for c in range(3):
                for j in range(LANE_TILES):
                    at = pl.multiple_of(c * spread + (x * LANE_TILES + j) * blocks, blocks)
                    over = pl.multiple_of((c * EDGE + x) * pitch + j * blocks, blocks)
                    value = jnp.where(flagged[j // 4], patch[pl.ds(over, blocks), :], rows[pl.ds(at, blocks), :])
                    to = pl.multiple_of(x * PLANE + j * 128, 128)
                    out[c, :, pl.ds(to, 128)] = value.astype(jnp.bfloat16)
            return carry

        lax.fori_loop(0, SPAN, one, 0)

    scatter(ORDER[0])
    scatter(ORDER[1])

    def forward(size):
        for k in everyone:
            ghost_arrival(k, size).wait_recv()
            relay_copy(k, size).start()

    def gather(size):
        for k in [0] + everyone:
            relay_copy(k, size).wait_recv()
            direct_arrival(k, size).wait_recv()

    on_level(0, forward)
    scatter(ORDER[2])
    on_level(1, gather)

    @pl.when(has_fine)
    def _():
        def expand(q, carry):
            pairs = []
            for corner in range(4):
                at = q * 8 + corner * 2
                pairs.append(jnp.concatenate([got_ghost[octants[0, at]], got_ghost[octants[0, at + 1]]], axis=1))
            full = jnp.dot(jnp.concatenate(pairs, axis=0), grow[...], preferred_element_type=jnp.float32)
            for corner in range(4):
                for c in range(3):
                    for jj in range(4):
                        for half in range(2):
                            x, j = corner // 2 * 16 + half * 8, corner % 2 * 4 + jj
                            to = (c * EDGE + x) * pitch + j * blocks + q
                            at = (corner * 12 + c * 4 + jj) * 8
                            patch[pl.ds(to, 8, stride=pitch), :] = full[at:at + 8, half * 128:(half + 1) * 128]
            return carry

        lax.fori_loop(0, blocks, expand, 0)

    for part in ORDER[:3]:
        finish(part)
    scatter(ORDER[3])
    finish(ORDER[3])

    @pl.when(not_last)
    def _():
        high(after).wait_send()

    @pl.when(not_first)
    def _():
        low(before).wait_send()

    for k in range(1, n):
        near(k).wait_send()
        for part in ORDER:
            block_copy(part, k).wait_send()

    @pl.when(has_coarse)
    def _():
        down().wait_send()

    def drain(size):
        for k in everyone:
            ghost_copy(k, size).wait_send()
        for k in [0] + everyone:
            relay_copy(k, size).wait_send()
            direct_copy(k, size).wait_send()

    on_level(0, drain)


def selection_tables():
    k = np.arange(1024)
    half, dx, odd, y, z = k // 512, k // 256 % 2, k // 128 % 2, k % 128 // 32, k % 32
    target = half * 64 + (2 * odd + y // 2) * 16 + z // 2
    shrink = np.where(target[:, None] == np.arange(128)[None, :], 0.125, 0.0)
    k = np.arange(256)
    oz, half, y, z = k // 128, k % 128 // 64, k % 64 // 16, k % 16
    target = half * 128 + y * 32 + oz * 16 + z
    grow = np.where(target[:, None] == np.arange(256)[None, :], 1.0, 0.0)
    return shrink, grow


def body(n, levels, vorticity, shift_field, new_index, parent_slot, flags):
    blocks, cells = vorticity.shape[2:]
    vort, shift = vorticity[0], shift_field[0]
    hbm = pl.BlockSpec(memory_space=pltpu.HBM)
    vmem = pl.BlockSpec(memory_space=pltpu.VMEM)
    bf16, f32, i32 = jnp.bfloat16, jnp.float32, jnp.int32
    dma, vm, smem = pltpu.SemaphoreType.DMA, pltpu.VMEM, pltpu.SMEM
    spread = EDGE * LANE_TILES * blocks
    piece = 3 * SPAN * LANE_TILES
    parts = EDGE // SPAN
    shrink, grow = selection_tables()
    out = pl.pallas_call(
        functools.partial(kernel, n, levels),
        out_shape=jax.ShapeDtypeStruct((3, blocks, cells), bf16),
        in_specs=[hbm] * 7,
        out_specs=vmem,
        scratch_shapes=[
            smem((1, blocks), i32), smem((1, blocks), i32), smem((1, blocks), i32),
            vm((4, blocks, cells), bf16), vm(shrink.shape, bf16), vm(grow.shape, bf16),
            vm((3 * spread, 128), f32), vm((3 * EDGE * (LANE_TILES + 1) * blocks, 128), f32),
            vm((parts, blocks, piece, 128), bf16), vm((4, blocks, 128), i32),
            *[vm((n, CAP, piece, 128), bf16)] * parts,
            *[vm((n * CAP, piece, 128), bf16)] * parts,
            vm((blocks, 96, 128), bf16), vm((n, CAP, 96, 128), bf16), vm((n * CAP, 96, 128), bf16),
            vm((n * CAP + 1, 96, 128), bf16),
            vm((128, 128), f32), vm((64, 128), bf16), vm((64, 128), bf16),
            vm((64, 128), bf16), vm((64, 128), bf16), vm((64, 128), f32), vm((64, 128), f32),
            vm((1, 128), i32), vm((n, 1, 128), i32), vm((n, 1, 128), i32),
            smem((n, 1, 128), i32), smem((n, 1, 128), i32),
            vm((1, 128), i32), smem((1, 128), i32), vm((1, 128), i32), smem((1, 128), i32),
            smem((CAP * n,), i32), smem((CAP * n,), i32),
            dma((6,)), dma((3,)), dma((6,)), dma((2,)), dma((2,)), dma((n,)), dma((n,)), dma, dma,
            dma((parts, n)), dma((parts, n)), dma((n,)), dma((n,)), dma((n,)), dma((n,)), dma((n,)), dma((n,)),
            pltpu.SemaphoreType.REGULAR, pltpu.SemaphoreType.REGULAR,
        ],
        compiler_params=pltpu.CompilerParams(
            collective_id=0, has_side_effects=True, vmem_limit_bytes=VMEM_LIMIT
        ),
        name="move",
    )(*[
        pltpu.with_memory_space_constraint(x, pltpu.HBM)
        for x in (new_index, parent_slot, flags, vort, shift, jnp.asarray(shrink, bf16), jnp.asarray(grow, bf16))
    ])
    return out[None]


def solution(mesh):
    placed = (
        P("lvl", None, "blk", None),
        P("lvl", "blk", None),
        P("lvl", "blk"),
        P("lvl", "blk"),
        P("lvl", "blk"),
    )
    step = functools.partial(body, mesh.shape["blk"], mesh.shape["lvl"])
    return jax.shard_map(
        step, mesh=mesh, in_specs=placed, out_specs=P("lvl", None, "blk", None), check_vma=False
    )
```

```python
import functools

import jax
import jax.numpy as jnp
import numpy as np
from jax import lax
from jax.experimental import pallas as pl
from jax.experimental.pallas import tpu as pltpu
from jax.sharding import PartitionSpec as P

MESH = pl.DeviceIdType.MESH
EDGE = 32
PLANE = EDGE * EDGE
LANE_TILES = PLANE // 128
CAP = 2
SPAN = 8
ORDER = (1, 2, 0, 3)
VMEM_LIMIT = 44 * 1024 * 1024
PIECES = ((4 * PLANE, 20 * PLANE), (20 * PLANE, 32 * PLANE), (0, 4 * PLANE))


def device(blk, lvl):
    return {"blk": blk, "lvl": lvl}


def remote(src, dst, send, recv, target):
    return pltpu.make_async_remote_copy(
        src_ref=src, dst_ref=dst, send_sem=send, recv_sem=recv, device_id=target, device_id_type=MESH
    )


def tap_weights(shifts):
    size = jnp.abs(shifts)
    rest = 1.0 - size
    size2 = size * size
    rest2 = rest * rest
    middle = 1.0 + size2 * (1.5 * size - 2.5)
    ahead = 1.0 + rest2 * (1.5 * rest - 2.5)
    behind = -0.5 * rest2 * size
    far = -0.5 * size2 * rest
    up = shifts >= 0.0
    return {
        -2: jnp.where(up, 0.0, far),
        -1: jnp.where(up, behind, ahead),
        0: middle,
        1: jnp.where(up, ahead, behind),
        2: jnp.where(up, far, 0.0),
    }


def split(value, size):
    if size & (size - 1) == 0:
        return lax.shift_right_logical(value, size.bit_length() - 1), lax.bitwise_and(value, size - 1)
    return lax.div(value, size), lax.rem(value, size)


def picks(keys, wanted):
    count, first, second = jnp.int32(0), jnp.int32(0), jnp.int32(0)
    for b, key in enumerate(keys):
        hit = key == wanted
        first = jnp.where(jnp.logical_and(hit, count == 0), b, first)
        second = jnp.where(jnp.logical_and(hit, count == 1), b, second)
        count = count + hit.astype(jnp.int32)
    return first, second


def shared_rows(lvl, levels):
    return 16 * min(max(round(6 * (lvl + 2) / (levels + 2)), 1), 5)


def kernel(n, levels, spots_in, parents_in, flags_in, vort_in, shift_in, shrink_in, grow_in, out,
           spots, parent_slot, flags, field, shrink, grow,
           rows, patch, whole, masks,
           send0, send1, send2, send3, got0, got1, got2, got3,
           small, ghost, relay, got_ghost,
           edge, edge_low, edge_high, below, above, halo_low, halo_high,
           tab, near_tabs, fine_tabs, near_local, fine_local, line, place, line2, octants,
           pick, pick_ghost,
           in_sem, index_sem, table_sem, halo_s, halo_r, near_s, near_r, down_s, down_r,
           block_s, block_r, ghost_s, ghost_r, relay_s, relay_r, direct_s, direct_r, plane_ready):
    me = lax.axis_index("blk")
    lvl = lax.axis_index("lvl")
    blocks = out.shape[1]
    spread = EDGE * LANE_TILES * blocks
    piece = SPAN * LANE_TILES
    pitch = (LANE_TILES + 1) * blocks
    coarse_level = jnp.maximum(lvl - 1, 0)
    fine_level = jnp.minimum(lvl + 1, levels - 1)
    sends, gots = (send0, send1, send2, send3), (got0, got1, got2, got3)
    after = device(lax.rem(me + 1, n), lvl)
    before = device(lax.rem(me + n - 1, n), lvl)
    below_level = device(me, coarse_level)
    has_coarse, has_fine = lvl > 0, lvl < levels - 1
    not_first, not_last = me > 0, me < n - 1

    others = range(1, n)
    partners = [lax.rem(me + k, n) for k in range(n)]
    sources = [lax.rem(me + n - k, n) for k in range(n)]

    barrier = pltpu.get_barrier_semaphore()

    def greet(blk, level):
        pl.semaphore_signal(barrier, inc=1, device_id=device(blk, level), device_id_type=MESH)

    for k in others:
        greet(partners[k], lvl)

    @pl.when(has_fine)
    def _():
        greet(me, fine_level)

    index_loads = [
        pltpu.make_async_copy(src, dst, index_sem.at[i])
        for i, (src, dst) in enumerate(((spots_in, spots), (parents_in, parent_slot), (flags_in, flags)))
    ]
    loads = []
    for i, (lo, hi) in enumerate(PIECES):
        part = pl.ds(lo, hi - lo)
        loads.append((
            pltpu.make_async_copy(shift_in.at[:, part], field.at[3, :, part], in_sem.at[2 * i]),
            pltpu.make_async_copy(vort_in.at[:, :, part], field.at[pl.ds(0, 3), :, part], in_sem.at[2 * i + 1]),
        ))
    constants = (
        pltpu.make_async_copy(shrink_in, shrink, table_sem.at[0]),
        pltpu.make_async_copy(grow_in, grow, table_sem.at[1]),
    )
    for copy in index_loads:
        copy.start()
    for pair in loads:
        for copy in pair:
            copy.start()
    for copy in constants:
        copy.start()

    sublane = lax.broadcasted_iota(jnp.int32, (blocks, 128), 0)
    lane = lax.broadcasted_iota(jnp.int32, (1, 128), 1)

    def tile(f, x, j):
        at = pl.multiple_of(x * PLANE + j * 128, 128)
        return field[f, :, pl.ds(at, 128)].astype(jnp.float32)

    def source_tile(f, x, j):
        if x < 0:
            edge_row = halo_low[pl.ds(f * 16 + (x + 2) * LANE_TILES + j, 1), :]
            return jnp.where(sublane == 0, edge_row, pltpu.roll(tile(f, x + EDGE, j), 1, 0))
        if x >= EDGE:
            edge_row = halo_high[pl.ds(f * 16 + (x - EDGE) * LANE_TILES + j, 1), :]
            return jnp.where(sublane == blocks - 1, edge_row, pltpu.roll(tile(f, x - EDGE, j), blocks - 1, 0))
        return tile(f, x, j)

    def remesh(part):
        x0, x1 = part * SPAN, (part + 1) * SPAN

        def chunk(j, carry):
            sums = [{}, {}, {}]
            for x in range(x0 - 2, x1 + 2):
                weights = tap_weights(source_tile(3, x, j))
                for c in range(3):
                    value = source_tile(c, x, j)
                    for offset in range(-2, 3):
                        to = x + offset
                        if x0 <= to < x1:
                            term = value * weights[offset]
                            sums[c][to] = sums[c][to] + term if to in sums[c] else term
                    if x0 <= x - 2:
                        at = c * spread + ((x - 2) * LANE_TILES + j) * blocks
                        rows[pl.ds(pl.multiple_of(at, blocks), blocks), :] = sums[c].pop(x - 2)
            return carry

        lax.fori_loop(0, LANE_TILES, chunk, 0)
        for b in range(blocks):
            for c in range(3):
                at = c * spread + x0 * LANE_TILES * blocks + b
                whole[part, b, c * piece:(c + 1) * piece, :] = rows[
                    pl.ds(at, piece, stride=blocks), :
                ].astype(jnp.bfloat16)

    def pack(part):
        def one(to, carry):
            for s in range(CAP):
                sends[part][to, s] = whole[part, pick[CAP * to + s]]
            return carry

        lax.fori_loop(0, n, one, 0)

    def keep(part):
        for s in range(CAP):
            gots[part][CAP * me + s] = whole[part, pick[CAP * me + s]]

    def block_copy(part, to):
        return remote(sends[part].at[to], gots[part].at[pl.ds(CAP * me, CAP)],
                      block_s.at[part, to], block_r.at[part, me], device(to, lvl))

    def block_arrival(part, source):
        return remote(sends[part].at[me], gots[part].at[pl.ds(CAP * source, CAP)],
                      block_s.at[part, source], block_r.at[part, source], before)

    def send_blocks(part):
        for k in others:
            block_copy(part, partners[k]).start()

    def near(k):
        return remote(tab, near_tabs.at[me], near_s.at[k], near_r.at[k], device(partners[k], lvl))

    def near_arrival(k):
        return remote(tab, near_tabs.at[sources[k]], near_s.at[k], near_r.at[k], before)

    def down():
        return remote(near_tabs, fine_tabs, down_s, down_r, below_level)

    def ghost_copy(k, size):
        part = pl.ds(0, size)
        return remote(ghost.at[partners[k], :, part], relay.at[pl.ds(CAP * me, CAP), part],
                      ghost_s.at[k], ghost_r.at[k], device(partners[k], lvl))

    def ghost_arrival(k, size):
        part = pl.ds(0, size)
        return remote(ghost.at[me, :, part], relay.at[pl.ds(CAP * sources[k], CAP), part],
                      ghost_s.at[k], ghost_r.at[k], before)

    def relay_copy(k, size):
        pair, part = pl.ds(CAP * sources[k], CAP), pl.ds(0, size)
        origin = ghost.at[me, :, part] if k == 0 else relay.at[pair, part]
        return remote(origin, got_ghost.at[pair, part], relay_s.at[k], relay_r.at[k], below_level)

    def direct_copy(k, size):
        part = pl.ds(size, 96 - size)
        return remote(ghost.at[partners[k], :, part], got_ghost.at[pl.ds(CAP * me, CAP), part],
                      direct_s.at[k], direct_r.at[k], device(partners[k], coarse_level))

    def direct_arrival(k, size):
        part = pl.ds(size, 96 - size)
        return remote(ghost.at[me, :, part], got_ghost.at[pl.ds(CAP * sources[k], CAP), part],
                      direct_s.at[k], direct_r.at[k], before)

    def on_level(shift, action):
        for level in range(1, levels):
            pl.when(lvl == level - shift)(functools.partial(action, shared_rows(level, levels)))

    def high(target):
        return remote(edge_high, below, halo_s.at[0], halo_r.at[0], target)

    def low(target):
        return remote(edge_low, above, halo_s.at[1], halo_r.at[1], target)

    for copy in index_loads:
        copy.wait()
    head = jnp.zeros((1, 128), jnp.int32)
    for part, ref in enumerate((spots, parent_slot, flags)):
        for b in range(blocks):
            head = jnp.where(lane == part * blocks + b, ref[0, b], head)
    tab[...] = head
    near_tabs[me] = head
    owners = [split(spots[0, b], blocks)[0] for b in range(blocks)]

    def choose(to, carry):
        first, second = picks(owners, to)
        pick[CAP * to] = first
        pick[CAP * to + 1] = second
        return carry

    lax.fori_loop(0, n, choose, 0)

    for copy in loads[0]:
        copy.wait()
    remesh(ORDER[0])
    pack(ORDER[0])
    for copy in loads[1] + loads[2]:
        copy.wait()

    def edges(j, carry):
        for f in range(4):
            for p in range(2):
                at = f * 16 + p * LANE_TILES + j
                edge[pl.ds(at, 1), :] = tile(f, p, j)[0:1, :]
                edge[pl.ds(64 + at, 1), :] = tile(f, EDGE - 2 + p, j)[blocks - 1:blocks, :]
        return carry

    lax.fori_loop(0, LANE_TILES, edges, 0)
    edge_low[...] = edge[0:64, :].astype(jnp.bfloat16)
    edge_high[...] = edge[64:128, :].astype(jnp.bfloat16)

    pl.semaphore_wait(barrier, n - 1 + has_coarse.astype(jnp.int32))

    @pl.when(not_last)
    def _():
        high(after).start()

    @pl.when(not_first)
    def _():
        low(before).start()

    for k in others:
        near(k).start()
    send_blocks(ORDER[0])
    keep(ORDER[0])
    remesh(ORDER[1])
    pack(ORDER[1])
    send_blocks(ORDER[1])
    keep(ORDER[1])

    @pl.when(not_last)
    def _():
        low(after).wait_recv()

    @pl.when(not_first)
    def _():
        high(before).wait_recv()

    halo_low[...] = jnp.where(not_first, below[...].astype(jnp.float32), 0.0)
    halo_high[...] = jnp.where(not_last, above[...].astype(jnp.float32), 0.0)
    for part in ORDER[2:]:
        remesh(part)
        pack(part)
        keep(part)

    for k in others:
        near_arrival(k).wait_recv()

    @pl.when(has_coarse)
    def _():
        down().start()

    fetch_near = pltpu.make_async_copy(near_tabs, near_local, table_sem.at[2])
    fetch_near.start()
    fetch_near.wait()
    for copy in constants:
        copy.wait()

    @pl.when(has_coarse)
    def _():
        parents = []
        for b in range(blocks):
            home, spot = split(spots[0, b], blocks)
            parents.append(split(near_local[home, 0, blocks + spot], 8 * blocks)[0])

        def choose_ghost(to, carry):
            first, second = picks(parents, to)
            pick_ghost[CAP * to] = first
            pick_ghost[CAP * to + 1] = second
            return carry

        lax.fori_loop(0, n, choose_ghost, 0)

        def restrict(b, carry):
            columns = []
            for half in range(2):
                for dx in range(2):
                    for odd in range(2):
                        parts = []
                        for c in range(3):
                            for jj in range(4):
                                x, j = half * 16 + dx, 2 * jj + odd
                                at = c * spread + (x * LANE_TILES + j) * blocks + b
                                parts.append(rows[pl.ds(at, 8, stride=2 * LANE_TILES * blocks), :])
                        columns.append(jnp.concatenate(parts, axis=0).astype(jnp.bfloat16))
            wide = jnp.concatenate(columns, axis=1)
            small[b] = jnp.dot(wide, shrink[...], preferred_element_type=jnp.float32).astype(jnp.bfloat16)
            return carry

        lax.fori_loop(0, blocks, restrict, 0)

        def pack_ghost(to, carry):
            for s in range(CAP):
                ghost[to, s] = small[pick_ghost[CAP * to + s]]
            return carry

        lax.fori_loop(0, n, pack_ghost, 0)

    def share(size):
        for k in others:
            ghost_copy(k, size).start()
        relay_copy(0, size).start()

    on_level(0, share)
    for part in ORDER[2:]:
        send_blocks(part)

    def settle_places(source, places):
        count = jnp.int32(0)
        for b in range(blocks):
            owner, spot = split(near_local[source, 0, b], blocks)
            mine = owner == me
            slot = CAP * source + jnp.minimum(count, CAP - 1)
            places = jnp.where(lane == jnp.where(mine, spot, -1), slot, places)
            count = count + mine.astype(jnp.int32)
        return places

    line[...] = lax.fori_loop(0, n, settle_places, jnp.zeros((1, 128), jnp.int32))
    fetch_place = pltpu.make_async_copy(line, place, table_sem.at[3])
    fetch_place.start()

    @pl.when(has_fine)
    def _():
        down().wait_recv()
        pl.semaphore_signal(plane_ready, inc=1, device_id=device(me, fine_level), device_id_type=MESH)
        fetch_fine = pltpu.make_async_copy(fine_tabs, fine_local, table_sem.at[4])
        fetch_fine.start()
        fetch_fine.wait()

    @pl.when(has_coarse)
    def _():
        pl.semaphore_wait(plane_ready, 1)

    def rest(size):
        for k in range(n):
            direct_copy(k, size).start()

    on_level(0, rest)
    empty = CAP * n

    def settle_octants(source, codes):
        count = jnp.int32(0)
        for b in range(blocks):
            home, spot = split(fine_local[source, 0, b], blocks)
            owner, code = split(fine_local[home, 0, blocks + spot], 8 * blocks)
            mine = owner == me
            hit = jnp.logical_and(mine, fine_local[home, 0, 2 * blocks + spot] == 1)
            slot = CAP * source + jnp.minimum(count, CAP - 1)
            codes = jnp.where(lane == jnp.where(hit, code, -1), slot, codes)
            count = count + mine.astype(jnp.int32)
        return codes

    rounds = jnp.where(has_fine, n, 0)
    line2[...] = lax.fori_loop(0, rounds, settle_octants, jnp.full((1, 128), empty, jnp.int32))
    fetch_octants = pltpu.make_async_copy(line2, octants, table_sem.at[5])
    fetch_octants.start()
    got_ghost[empty] = jnp.zeros(got_ghost.shape[1:], jnp.bfloat16)
    fetch_place.wait()
    fetch_octants.wait()

    wide_lane = lax.broadcasted_iota(jnp.int32, (blocks, 128), 1)
    deep = lax.bitwise_and(wide_lane, 16) != 0
    for corner in range(4):
        mask = jnp.zeros((blocks, 128), jnp.int32)
        for q in range(blocks):
            near_half = (octants[0, q * 8 + corner * 2] < empty).astype(jnp.int32)
            far_half = (octants[0, q * 8 + corner * 2 + 1] < empty).astype(jnp.int32)
            mask = jnp.where(sublane == q, jnp.where(deep, far_half, near_half), mask)
        masks[corner] = mask

    def scatter(part):
        for k in others:
            block_arrival(part, sources[k]).wait_recv()

        def one(q, carry):
            block = gots[part][place[0, q]].astype(jnp.float32)
            for c in range(3):
                at = c * spread + part * piece * blocks + q
                rows[pl.ds(at, piece, stride=blocks), :] = block[c * piece:(c + 1) * piece, :]
            return carry

        lax.fori_loop(0, blocks, one, 0)

    def finish(part):
        flagged = [masks[(part * SPAN // 16) * 2 + oy] != 0 for oy in range(2)]

        def one(i, carry):
            x = part * SPAN + i
            for c in range(3):
                for j in range(LANE_TILES):
                    at = pl.multiple_of(c * spread + (x * LANE_TILES + j) * blocks, blocks)
                    over = pl.multiple_of((c * EDGE + x) * pitch + j * blocks, blocks)
                    value = jnp.where(flagged[j // 4], patch[pl.ds(over, blocks), :], rows[pl.ds(at, blocks), :])
                    to = pl.multiple_of(x * PLANE + j * 128, 128)
                    out[c, :, pl.ds(to, 128)] = value.astype(jnp.bfloat16)
            return carry

        lax.fori_loop(0, SPAN, one, 0)

    scatter(ORDER[0])
    scatter(ORDER[1])

    def forward(size):
        for k in others:
            ghost_arrival(k, size).wait_recv()
            relay_copy(k, size).start()

    def gather(size):
        for k in range(n):
            relay_copy(k, size).wait_recv()
            direct_arrival(k, size).wait_recv()

    on_level(0, forward)
    scatter(ORDER[2])
    on_level(1, gather)

    @pl.when(has_fine)
    def _():
        def expand(q, carry):
            pairs = []
            for corner in range(4):
                at = q * 8 + corner * 2
                pairs.append(jnp.concatenate([got_ghost[octants[0, at]], got_ghost[octants[0, at + 1]]], axis=1))
            full = jnp.dot(jnp.concatenate(pairs, axis=0), grow[...], preferred_element_type=jnp.float32)
            for corner in range(4):
                for c in range(3):
                    for jj in range(4):
                        for half in range(2):
                            x, j = corner // 2 * 16 + half * 8, corner % 2 * 4 + jj
                            to = (c * EDGE + x) * pitch + j * blocks + q
                            at = (corner * 12 + c * 4 + jj) * 8
                            patch[pl.ds(to, 8, stride=pitch), :] = full[at:at + 8, half * 128:(half + 1) * 128]
            return carry

        lax.fori_loop(0, blocks, expand, 0)

    for part in ORDER[:3]:
        finish(part)
    scatter(ORDER[3])
    finish(ORDER[3])

    @pl.when(not_last)
    def _():
        high(after).wait_send()

    @pl.when(not_first)
    def _():
        low(before).wait_send()

    for k in others:
        near(k).wait_send()
        for part in ORDER:
            block_copy(part, partners[k]).wait_send()

    @pl.when(has_coarse)
    def _():
        down().wait_send()

    def drain(size):
        for k in others:
            ghost_copy(k, size).wait_send()
        for k in range(n):
            relay_copy(k, size).wait_send()
            direct_copy(k, size).wait_send()

    on_level(0, drain)


def selection_tables():
    k = np.arange(1024)
    half, dx, odd, y, z = k // 512, k // 256 % 2, k // 128 % 2, k % 128 // 32, k % 32
    target = half * 64 + (2 * odd + y // 2) * 16 + z // 2
    shrink = np.where(target[:, None] == np.arange(128)[None, :], 0.125, 0.0)
    k = np.arange(256)
    oz, half, y, z = k // 128, k % 128 // 64, k % 64 // 16, k % 16
    target = half * 128 + y * 32 + oz * 16 + z
    grow = np.where(target[:, None] == np.arange(256)[None, :], 1.0, 0.0)
    return shrink, grow


def body(n, levels, vorticity, shift_field, new_index, parent_slot, flags):
    blocks, cells = vorticity.shape[2:]
    vort, shift = vorticity[0], shift_field[0]
    hbm = pl.BlockSpec(memory_space=pltpu.HBM)
    vmem = pl.BlockSpec(memory_space=pltpu.VMEM)
    bf16, f32, i32 = jnp.bfloat16, jnp.float32, jnp.int32
    dma, vm, smem = pltpu.SemaphoreType.DMA, pltpu.VMEM, pltpu.SMEM
    spread = EDGE * LANE_TILES * blocks
    piece = 3 * SPAN * LANE_TILES
    parts = EDGE // SPAN
    shrink, grow = selection_tables()
    out = pl.pallas_call(
        functools.partial(kernel, n, levels),
        out_shape=jax.ShapeDtypeStruct((3, blocks, cells), bf16),
        in_specs=[hbm] * 7,
        out_specs=vmem,
        scratch_shapes=[
            smem((1, blocks), i32), smem((1, blocks), i32), smem((1, blocks), i32),
            vm((4, blocks, cells), bf16), vm(shrink.shape, bf16), vm(grow.shape, bf16),
            vm((3 * spread, 128), f32), vm((3 * EDGE * (LANE_TILES + 1) * blocks, 128), f32),
            vm((parts, blocks, piece, 128), bf16), vm((4, blocks, 128), i32),
            *[vm((n, CAP, piece, 128), bf16)] * parts,
            *[vm((n * CAP, piece, 128), bf16)] * parts,
            vm((blocks, 96, 128), bf16), vm((n, CAP, 96, 128), bf16), vm((n * CAP, 96, 128), bf16),
            vm((n * CAP + 1, 96, 128), bf16),
            vm((128, 128), f32), vm((64, 128), bf16), vm((64, 128), bf16),
            vm((64, 128), bf16), vm((64, 128), bf16), vm((64, 128), f32), vm((64, 128), f32),
            vm((1, 128), i32), vm((n, 1, 128), i32), vm((n, 1, 128), i32),
            smem((n, 1, 128), i32), smem((n, 1, 128), i32),
            vm((1, 128), i32), smem((1, 128), i32), vm((1, 128), i32), smem((1, 128), i32),
            smem((CAP * n,), i32), smem((CAP * n,), i32),
            dma((6,)), dma((3,)), dma((6,)), dma((2,)), dma((2,)), dma((n,)), dma((n,)), dma, dma,
            dma((parts, n)), dma((parts, n)), dma((n,)), dma((n,)), dma((n,)), dma((n,)), dma((n,)), dma((n,)),
            pltpu.SemaphoreType.REGULAR,
        ],
        compiler_params=pltpu.CompilerParams(
            collective_id=0, has_side_effects=True, vmem_limit_bytes=VMEM_LIMIT
        ),
        name="move",
    )(*[
        pltpu.with_memory_space_constraint(x, pltpu.HBM)
        for x in (new_index, parent_slot, flags, vort, shift, jnp.asarray(shrink, bf16), jnp.asarray(grow, bf16))
    ])
    return out[None]


def solution(mesh):
    placed = (
        P("lvl", None, "blk", None),
        P("lvl", "blk", None),
        P("lvl", "blk"),
        P("lvl", "blk"),
        P("lvl", "blk"),
    )
    step = functools.partial(body, mesh.shape["blk"], mesh.shape["lvl"])
    return jax.shard_map(
        step, mesh=mesh, in_specs=placed, out_specs=P("lvl", None, "blk", None), check_vma=False
    )
```

```python
import functools

import jax
import jax.numpy as jnp
import numpy as np
from jax import lax
from jax.experimental import pallas as pl
from jax.experimental.pallas import tpu as pltpu
from jax.sharding import PartitionSpec as P

MESH = pl.DeviceIdType.MESH
EDGE = 32
PLANE = EDGE * EDGE
LANE_TILES = PLANE // 128
CAP = 2
PARTS = ((8, 12), (12, 28), (0, 8), (28, 32))
VMEM_LIMIT = 44 * 1024 * 1024
PIECES = ((6 * PLANE, 14 * PLANE), (14 * PLANE, 32 * PLANE), (0, 6 * PLANE))


def device(blk, lvl):
    return {"blk": blk, "lvl": lvl}


def remote(src, dst, send, recv, target):
    return pltpu.make_async_remote_copy(
        src_ref=src, dst_ref=dst, send_sem=send, recv_sem=recv, device_id=target, device_id_type=MESH
    )


def tap_weights(shifts):
    size = jnp.abs(shifts)
    rest = 1.0 - size
    size2 = size * size
    rest2 = rest * rest
    middle = 1.0 + size2 * (1.5 * size - 2.5)
    ahead = 1.0 + rest2 * (1.5 * rest - 2.5)
    behind = -0.5 * rest2 * size
    far = -0.5 * size2 * rest
    up = shifts >= 0.0
    return {
        -2: jnp.where(up, 0.0, far),
        -1: jnp.where(up, behind, ahead),
        0: middle,
        1: jnp.where(up, ahead, behind),
        2: jnp.where(up, far, 0.0),
    }


def split(value, size):
    if size & (size - 1) == 0:
        return lax.shift_right_logical(value, size.bit_length() - 1), lax.bitwise_and(value, size - 1)
    return lax.div(value, size), lax.rem(value, size)


def picks(keys, wanted):
    count, first, second = jnp.int32(0), jnp.int32(0), jnp.int32(0)
    for b, key in enumerate(keys):
        hit = key == wanted
        first = jnp.where(jnp.logical_and(hit, count == 0), b, first)
        second = jnp.where(jnp.logical_and(hit, count == 1), b, second)
        count = count + hit.astype(jnp.int32)
    return first, second


def shared_rows(lvl, levels):
    return 16 * min(max(round(6 * (lvl + 2) / (levels + 2)), 1), 5)


def kernel(n, levels, spots_in, parents_in, flags_in, vort_in, shift_in, shrink_in, grow_in, out,
           spots, parent_slot, flags, field, shrink, grow,
           rows, patch, whole0, whole1, whole2, whole3, masks,
           send0, send1, send2, send3, got0, got1, got2, got3,
           small, ghost, relay, got_ghost,
           edge, edge_low, edge_high, below, above, halo_low, halo_high,
           tab, near_tabs, fine_tabs, near_local, fine_local, line, place, line2, octants,
           pick, pick_ghost,
           in_sem, index_sem, table_sem, halo_s, halo_r, near_s, near_r, down_s, down_r,
           block_s, block_r, ghost_s, ghost_r, relay_s, relay_r, direct_s, direct_r, plane_ready):
    me = lax.axis_index("blk")
    lvl = lax.axis_index("lvl")
    blocks = out.shape[1]
    spread = EDGE * LANE_TILES * blocks
    pitch = (LANE_TILES + 1) * blocks
    coarse_level = jnp.maximum(lvl - 1, 0)
    fine_level = jnp.minimum(lvl + 1, levels - 1)
    pieces = [(x1 - x0) * LANE_TILES for x0, x1 in PARTS]
    wholes = (whole0, whole1, whole2, whole3)
    sends, gots = (send0, send1, send2, send3), (got0, got1, got2, got3)
    after = device(lax.rem(me + 1, n), lvl)
    before = device(lax.rem(me + n - 1, n), lvl)
    below_level = device(me, coarse_level)
    has_coarse, has_fine = lvl > 0, lvl < levels - 1
    not_first, not_last = me > 0, me < n - 1

    others = range(1, n)
    partners = [lax.rem(me + k, n) for k in range(n)]
    sources = [lax.rem(me + n - k, n) for k in range(n)]

    barrier = pltpu.get_barrier_semaphore()

    def greet(blk, level):
        pl.semaphore_signal(barrier, inc=1, device_id=device(blk, level), device_id_type=MESH)

    for k in others:
        greet(partners[k], lvl)

    @pl.when(has_fine)
    def _():
        greet(me, fine_level)

    index_loads = [
        pltpu.make_async_copy(src, dst, index_sem.at[i])
        for i, (src, dst) in enumerate(((spots_in, spots), (parents_in, parent_slot), (flags_in, flags)))
    ]
    loads = []
    for i, (lo, hi) in enumerate(PIECES):
        part = pl.ds(lo, hi - lo)
        loads.append((
            pltpu.make_async_copy(shift_in.at[:, part], field.at[3, :, part], in_sem.at[2 * i]),
            pltpu.make_async_copy(vort_in.at[:, :, part], field.at[pl.ds(0, 3), :, part], in_sem.at[2 * i + 1]),
        ))
    constants = (
        pltpu.make_async_copy(shrink_in, shrink, table_sem.at[0]),
        pltpu.make_async_copy(grow_in, grow, table_sem.at[1]),
    )
    for copy in loads[0]:
        copy.start()
    for copy in index_loads:
        copy.start()
    for copy in loads[1] + loads[2]:
        copy.start()
    for copy in constants:
        copy.start()

    sublane = lax.broadcasted_iota(jnp.int32, (blocks, 128), 0)
    lane = lax.broadcasted_iota(jnp.int32, (1, 128), 1)

    def tile(f, x, j):
        at = pl.multiple_of(x * PLANE + j * 128, 128)
        return field[f, :, pl.ds(at, 128)].astype(jnp.float32)

    def source_tile(f, x, j):
        if x < 0:
            edge_row = halo_low[pl.ds(f * 16 + (x + 2) * LANE_TILES + j, 1), :]
            return jnp.where(sublane == 0, edge_row, pltpu.roll(tile(f, x + EDGE, j), 1, 0))
        if x >= EDGE:
            edge_row = halo_high[pl.ds(f * 16 + (x - EDGE) * LANE_TILES + j, 1), :]
            return jnp.where(sublane == blocks - 1, edge_row, pltpu.roll(tile(f, x - EDGE, j), blocks - 1, 0))
        return tile(f, x, j)

    def remesh(part):
        (x0, x1), piece = PARTS[part], pieces[part]

        def chunk(j, carry):
            sums = [{}, {}, {}]
            for x in range(x0 - 2, x1 + 2):
                weights = tap_weights(source_tile(3, x, j))
                for c in range(3):
                    value = source_tile(c, x, j)
                    for offset in range(-2, 3):
                        to = x + offset
                        if x0 <= to < x1:
                            term = value * weights[offset]
                            sums[c][to] = sums[c][to] + term if to in sums[c] else term
                    if x0 <= x - 2:
                        at = c * spread + ((x - 2) * LANE_TILES + j) * blocks
                        rows[pl.ds(pl.multiple_of(at, blocks), blocks), :] = sums[c].pop(x - 2)
            return carry

        lax.fori_loop(0, LANE_TILES, chunk, 0)
        for b in range(blocks):
            for c in range(3):
                at = c * spread + x0 * LANE_TILES * blocks + b
                wholes[part][b, c * piece:(c + 1) * piece, :] = rows[
                    pl.ds(at, piece, stride=blocks), :
                ].astype(jnp.bfloat16)

    def pack(part):
        def one(to, carry):
            for s in range(CAP):
                sends[part][to, s] = wholes[part][pick[CAP * to + s]]
            return carry

        lax.fori_loop(0, n, one, 0)

    def keep(part):
        for s in range(CAP):
            gots[part][CAP * me + s] = wholes[part][pick[CAP * me + s]]

    def block_copy(part, to):
        return remote(sends[part].at[to], gots[part].at[pl.ds(CAP * me, CAP)],
                      block_s.at[part, to], block_r.at[part, me], device(to, lvl))

    def block_arrival(part, source):
        return remote(sends[part].at[me], gots[part].at[pl.ds(CAP * source, CAP)],
                      block_s.at[part, source], block_r.at[part, source], before)

    def send_blocks(part):
        for k in others:
            block_copy(part, partners[k]).start()

    def near(k):
        return remote(tab, near_tabs.at[me], near_s.at[k], near_r.at[k], device(partners[k], lvl))

    def near_arrival(k):
        return remote(tab, near_tabs.at[sources[k]], near_s.at[k], near_r.at[k], before)

    def down():
        return remote(near_tabs, fine_tabs, down_s, down_r, below_level)

    def ghost_copy(k, size):
        part = pl.ds(0, size)
        return remote(ghost.at[partners[k], :, part], relay.at[pl.ds(CAP * me, CAP), part],
                      ghost_s.at[k], ghost_r.at[k], device(partners[k], lvl))

    def ghost_arrival(k, size):
        part = pl.ds(0, size)
        return remote(ghost.at[me, :, part], relay.at[pl.ds(CAP * sources[k], CAP), part],
                      ghost_s.at[k], ghost_r.at[k], before)

    def relay_copy(k, size):
        pair, part = pl.ds(CAP * sources[k], CAP), pl.ds(0, size)
        origin = ghost.at[me, :, part] if k == 0 else relay.at[pair, part]
        return remote(origin, got_ghost.at[pair, part], relay_s.at[k], relay_r.at[k], below_level)

    def direct_copy(k, size):
        part = pl.ds(size, 96 - size)
        return remote(ghost.at[partners[k], :, part], got_ghost.at[pl.ds(CAP * me, CAP), part],
                      direct_s.at[k], direct_r.at[k], device(partners[k], coarse_level))

    def direct_arrival(k, size):
        part = pl.ds(size, 96 - size)
        return remote(ghost.at[me, :, part], got_ghost.at[pl.ds(CAP * sources[k], CAP), part],
                      direct_s.at[k], direct_r.at[k], before)

    def on_level(shift, action):
        for level in range(1, levels):
            pl.when(lvl == level - shift)(functools.partial(action, shared_rows(level, levels)))

    def high(target):
        return remote(edge_high, below, halo_s.at[0], halo_r.at[0], target)

    def low(target):
        return remote(edge_low, above, halo_s.at[1], halo_r.at[1], target)

    for copy in index_loads:
        copy.wait()
    head = jnp.zeros((1, 128), jnp.int32)
    for part, ref in enumerate((spots, parent_slot, flags)):
        for b in range(blocks):
            head = jnp.where(lane == part * blocks + b, ref[0, b], head)
    tab[...] = head
    near_tabs[me] = head
    owners = [split(spots[0, b], blocks)[0] for b in range(blocks)]

    def choose(to, carry):
        first, second = picks(owners, to)
        pick[CAP * to] = first
        pick[CAP * to + 1] = second
        return carry

    lax.fori_loop(0, n, choose, 0)

    for copy in loads[0]:
        copy.wait()
    remesh(0)
    pack(0)
    for copy in loads[1] + loads[2]:
        copy.wait()

    def edges(j, carry):
        for f in range(4):
            for p in range(2):
                at = f * 16 + p * LANE_TILES + j
                edge[pl.ds(at, 1), :] = tile(f, p, j)[0:1, :]
                edge[pl.ds(64 + at, 1), :] = tile(f, EDGE - 2 + p, j)[blocks - 1:blocks, :]
        return carry

    lax.fori_loop(0, LANE_TILES, edges, 0)
    edge_low[...] = edge[0:64, :].astype(jnp.bfloat16)
    edge_high[...] = edge[64:128, :].astype(jnp.bfloat16)

    pl.semaphore_wait(barrier, n - 1 + has_coarse.astype(jnp.int32))

    send_blocks(0)

    @pl.when(not_last)
    def _():
        high(after).start()

    @pl.when(not_first)
    def _():
        low(before).start()

    for k in others:
        near(k).start()
    keep(0)
    remesh(1)
    pack(1)
    send_blocks(1)
    keep(1)

    @pl.when(not_last)
    def _():
        low(after).wait_recv()

    @pl.when(not_first)
    def _():
        high(before).wait_recv()

    halo_low[...] = jnp.where(not_first, below[...].astype(jnp.float32), 0.0)
    halo_high[...] = jnp.where(not_last, above[...].astype(jnp.float32), 0.0)
    for part in (2, 3):
        remesh(part)
        pack(part)
        keep(part)

    for k in others:
        near_arrival(k).wait_recv()

    @pl.when(has_coarse)
    def _():
        down().start()

    fetch_near = pltpu.make_async_copy(near_tabs, near_local, table_sem.at[2])
    fetch_near.start()
    fetch_near.wait()
    for copy in constants:
        copy.wait()

    @pl.when(has_coarse)
    def _():
        parents = []
        for b in range(blocks):
            home, spot = split(spots[0, b], blocks)
            parents.append(split(near_local[home, 0, blocks + spot], 8 * blocks)[0])

        def choose_ghost(to, carry):
            first, second = picks(parents, to)
            pick_ghost[CAP * to] = first
            pick_ghost[CAP * to + 1] = second
            return carry

        lax.fori_loop(0, n, choose_ghost, 0)

        def restrict(b, carry):
            columns = []
            for half in range(2):
                for dx in range(2):
                    for odd in range(2):
                        parts = []
                        for c in range(3):
                            for jj in range(4):
                                x, j = half * 16 + dx, 2 * jj + odd
                                at = c * spread + (x * LANE_TILES + j) * blocks + b
                                parts.append(rows[pl.ds(at, 8, stride=2 * LANE_TILES * blocks), :])
                        columns.append(jnp.concatenate(parts, axis=0).astype(jnp.bfloat16))
            wide = jnp.concatenate(columns, axis=1)
            small[b] = jnp.dot(wide, shrink[...], preferred_element_type=jnp.float32).astype(jnp.bfloat16)
            return carry

        lax.fori_loop(0, blocks, restrict, 0)

        def pack_ghost(to, carry):
            for s in range(CAP):
                ghost[to, s] = small[pick_ghost[CAP * to + s]]
            return carry

        lax.fori_loop(0, n, pack_ghost, 0)

    def share(size):
        for k in others:
            ghost_copy(k, size).start()
        relay_copy(0, size).start()

    on_level(0, share)
    for part in (2, 3):
        send_blocks(part)

    def settle_places(source, places):
        count = jnp.int32(0)
        for b in range(blocks):
            owner, spot = split(near_local[source, 0, b], blocks)
            mine = owner == me
            slot = CAP * source + jnp.minimum(count, CAP - 1)
            places = jnp.where(lane == jnp.where(mine, spot, -1), slot, places)
            count = count + mine.astype(jnp.int32)
        return places

    line[...] = lax.fori_loop(0, n, settle_places, jnp.zeros((1, 128), jnp.int32))
    fetch_place = pltpu.make_async_copy(line, place, table_sem.at[3])
    fetch_place.start()

    @pl.when(has_fine)
    def _():
        down().wait_recv()
        pl.semaphore_signal(plane_ready, inc=1, device_id=device(me, fine_level), device_id_type=MESH)
        fetch_fine = pltpu.make_async_copy(fine_tabs, fine_local, table_sem.at[4])
        fetch_fine.start()
        fetch_fine.wait()

    @pl.when(has_coarse)
    def _():
        pl.semaphore_wait(plane_ready, 1)

    def rest(size):
        for k in range(n):
            direct_copy(k, size).start()

    on_level(0, rest)
    empty = CAP * n

    def settle_octants(source, codes):
        count = jnp.int32(0)
        for b in range(blocks):
            home, spot = split(fine_local[source, 0, b], blocks)
            owner, code = split(fine_local[home, 0, blocks + spot], 8 * blocks)
            mine = owner == me
            hit = jnp.logical_and(mine, fine_local[home, 0, 2 * blocks + spot] == 1)
            slot = CAP * source + jnp.minimum(count, CAP - 1)
            codes = jnp.where(lane == jnp.where(hit, code, -1), slot, codes)
            count = count + mine.astype(jnp.int32)
        return codes

    rounds = jnp.where(has_fine, n, 0)
    line2[...] = lax.fori_loop(0, rounds, settle_octants, jnp.full((1, 128), empty, jnp.int32))
    fetch_octants = pltpu.make_async_copy(line2, octants, table_sem.at[5])
    fetch_octants.start()
    got_ghost[empty] = jnp.zeros(got_ghost.shape[1:], jnp.bfloat16)
    fetch_place.wait()
    fetch_octants.wait()

    wide_lane = lax.broadcasted_iota(jnp.int32, (blocks, 128), 1)
    deep = lax.bitwise_and(wide_lane, 16) != 0
    for corner in range(4):
        mask = jnp.zeros((blocks, 128), jnp.int32)
        for q in range(blocks):
            near_half = (octants[0, q * 8 + corner * 2] < empty).astype(jnp.int32)
            far_half = (octants[0, q * 8 + corner * 2 + 1] < empty).astype(jnp.int32)
            mask = jnp.where(sublane == q, jnp.where(deep, far_half, near_half), mask)
        masks[corner] = mask

    def scatter(part):
        for k in others:
            block_arrival(part, sources[k]).wait_recv()

        piece = pieces[part]

        def one(q, carry):
            block = gots[part][place[0, q]].astype(jnp.float32)
            for c in range(3):
                at = c * spread + PARTS[part][0] * LANE_TILES * blocks + q
                rows[pl.ds(at, piece, stride=blocks), :] = block[c * piece:(c + 1) * piece, :]
            return carry

        lax.fori_loop(0, blocks, one, 0)

    def finish(part):
        def one(x, carry):
            flagged = [masks[2 * lax.div(x, 16) + oy] != 0 for oy in range(2)]
            for c in range(3):
                for j in range(LANE_TILES):
                    at = pl.multiple_of(c * spread + (x * LANE_TILES + j) * blocks, blocks)
                    over = pl.multiple_of((c * EDGE + x) * pitch + j * blocks, blocks)
                    value = jnp.where(flagged[j // 4], patch[pl.ds(over, blocks), :], rows[pl.ds(at, blocks), :])
                    to = pl.multiple_of(x * PLANE + j * 128, 128)
                    out[c, :, pl.ds(to, 128)] = value.astype(jnp.bfloat16)
            return carry

        lax.fori_loop(*PARTS[part], one, 0)

    scatter(0)
    scatter(1)

    def forward(size):
        for k in others:
            ghost_arrival(k, size).wait_recv()
            relay_copy(k, size).start()

    def gather(size):
        for k in range(n):
            relay_copy(k, size).wait_recv()
            direct_arrival(k, size).wait_recv()

    on_level(0, forward)
    scatter(2)
    on_level(1, gather)

    @pl.when(has_fine)
    def _():
        def expand(q, carry):
            pairs = []
            for corner in range(4):
                at = q * 8 + corner * 2
                pairs.append(jnp.concatenate([got_ghost[octants[0, at]], got_ghost[octants[0, at + 1]]], axis=1))
            full = jnp.dot(jnp.concatenate(pairs, axis=0), grow[...], preferred_element_type=jnp.float32)
            for corner in range(4):
                for c in range(3):
                    for jj in range(4):
                        for half in range(2):
                            x, j = corner // 2 * 16 + half * 8, corner % 2 * 4 + jj
                            to = (c * EDGE + x) * pitch + j * blocks + q
                            at = (corner * 12 + c * 4 + jj) * 8
                            patch[pl.ds(to, 8, stride=pitch), :] = full[at:at + 8, half * 128:(half + 1) * 128]
            return carry

        lax.fori_loop(0, blocks, expand, 0)

    for part in (0, 1, 2):
        finish(part)
    scatter(3)
    finish(3)

    @pl.when(not_last)
    def _():
        high(after).wait_send()

    @pl.when(not_first)
    def _():
        low(before).wait_send()

    for k in others:
        near(k).wait_send()
        for part in range(len(PARTS)):
            block_copy(part, partners[k]).wait_send()

    @pl.when(has_coarse)
    def _():
        down().wait_send()

    def drain(size):
        for k in others:
            ghost_copy(k, size).wait_send()
        for k in range(n):
            relay_copy(k, size).wait_send()
            direct_copy(k, size).wait_send()

    on_level(0, drain)


def selection_tables():
    k = np.arange(1024)
    half, dx, odd, y, z = k // 512, k // 256 % 2, k // 128 % 2, k % 128 // 32, k % 32
    target = half * 64 + (2 * odd + y // 2) * 16 + z // 2
    shrink = np.where(target[:, None] == np.arange(128)[None, :], 0.125, 0.0)
    k = np.arange(256)
    oz, half, y, z = k // 128, k % 128 // 64, k % 64 // 16, k % 16
    target = half * 128 + y * 32 + oz * 16 + z
    grow = np.where(target[:, None] == np.arange(256)[None, :], 1.0, 0.0)
    return shrink, grow


def body(n, levels, vorticity, shift_field, new_index, parent_slot, flags):
    blocks, cells = vorticity.shape[2:]
    vort, shift = vorticity[0], shift_field[0]
    hbm = pl.BlockSpec(memory_space=pltpu.HBM)
    vmem = pl.BlockSpec(memory_space=pltpu.VMEM)
    bf16, f32, i32 = jnp.bfloat16, jnp.float32, jnp.int32
    dma, vm, smem = pltpu.SemaphoreType.DMA, pltpu.VMEM, pltpu.SMEM
    spread = EDGE * LANE_TILES * blocks
    pieces = [3 * (x1 - x0) * LANE_TILES for x0, x1 in PARTS]
    parts = len(PARTS)
    shrink, grow = selection_tables()
    out = pl.pallas_call(
        functools.partial(kernel, n, levels),
        out_shape=jax.ShapeDtypeStruct((3, blocks, cells), bf16),
        in_specs=[hbm] * 7,
        out_specs=vmem,
        scratch_shapes=[
            smem((1, blocks), i32), smem((1, blocks), i32), smem((1, blocks), i32),
            vm((4, blocks, cells), bf16), vm(shrink.shape, bf16), vm(grow.shape, bf16),
            vm((3 * spread, 128), f32), vm((3 * EDGE * (LANE_TILES + 1) * blocks, 128), f32),
            *[vm((blocks, piece, 128), bf16) for piece in pieces], vm((4, blocks, 128), i32),
            *[vm((n, CAP, piece, 128), bf16) for piece in pieces],
            *[vm((n * CAP, piece, 128), bf16) for piece in pieces],
            vm((blocks, 96, 128), bf16), vm((n, CAP, 96, 128), bf16), vm((n * CAP, 96, 128), bf16),
            vm((n * CAP + 1, 96, 128), bf16),
            vm((128, 128), f32), vm((64, 128), bf16), vm((64, 128), bf16),
            vm((64, 128), bf16), vm((64, 128), bf16), vm((64, 128), f32), vm((64, 128), f32),
            vm((1, 128), i32), vm((n, 1, 128), i32), vm((n, 1, 128), i32),
            smem((n, 1, 128), i32), smem((n, 1, 128), i32),
            vm((1, 128), i32), smem((1, 128), i32), vm((1, 128), i32), smem((1, 128), i32),
            smem((CAP * n,), i32), smem((CAP * n,), i32),
            dma((6,)), dma((3,)), dma((6,)), dma((2,)), dma((2,)), dma((n,)), dma((n,)), dma, dma,
            dma((parts, n)), dma((parts, n)), dma((n,)), dma((n,)), dma((n,)), dma((n,)), dma((n,)), dma((n,)),
            pltpu.SemaphoreType.REGULAR,
        ],
        compiler_params=pltpu.CompilerParams(
            collective_id=0, has_side_effects=True, vmem_limit_bytes=VMEM_LIMIT
        ),
        name="move",
    )(*[
        pltpu.with_memory_space_constraint(x, pltpu.HBM)
        for x in (new_index, parent_slot, flags, vort, shift, jnp.asarray(shrink, bf16), jnp.asarray(grow, bf16))
    ])
    return out[None]


def solution(mesh):
    placed = (
        P("lvl", None, "blk", None),
        P("lvl", "blk", None),
        P("lvl", "blk"),
        P("lvl", "blk"),
        P("lvl", "blk"),
    )
    step = functools.partial(body, mesh.shape["blk"], mesh.shape["lvl"])
    return jax.shard_map(
        step, mesh=mesh, in_specs=placed, out_specs=P("lvl", None, "blk", None), check_vma=False
    )
```

```python
import functools

import jax
import jax.numpy as jnp
import numpy as np
from jax import lax
from jax.experimental import pallas as pl
from jax.experimental.pallas import tpu as pltpu
from jax.sharding import PartitionSpec as P

MESH = pl.DeviceIdType.MESH
EDGE = 32
PLANE = EDGE * EDGE
LANE_TILES = PLANE // 128
CAP = 2
PARTS = ((4, 8), (8, 20), (20, 32), (0, 4))
VMEM_LIMIT = 44 * 1024 * 1024
PIECES = ((2 * PLANE, 10 * PLANE), (10 * PLANE, 32 * PLANE), (0, 2 * PLANE))


def device(blk, lvl):
    return {"blk": blk, "lvl": lvl}


def remote(src, dst, send, recv, target):
    return pltpu.make_async_remote_copy(
        src_ref=src, dst_ref=dst, send_sem=send, recv_sem=recv, device_id=target, device_id_type=MESH
    )


def tap_weights(shifts):
    size = jnp.abs(shifts)
    rest = 1.0 - size
    size2 = size * size
    rest2 = rest * rest
    middle = 1.0 + size2 * (1.5 * size - 2.5)
    ahead = 1.0 + rest2 * (1.5 * rest - 2.5)
    behind = -0.5 * rest2 * size
    far = -0.5 * size2 * rest
    up = shifts >= 0.0
    return {
        -2: jnp.where(up, 0.0, far),
        -1: jnp.where(up, behind, ahead),
        0: middle,
        1: jnp.where(up, ahead, behind),
        2: jnp.where(up, far, 0.0),
    }


def split(value, size):
    if size & (size - 1) == 0:
        return lax.shift_right_logical(value, size.bit_length() - 1), lax.bitwise_and(value, size - 1)
    return lax.div(value, size), lax.rem(value, size)


def picks(keys, wanted):
    count, first, second = jnp.int32(0), jnp.int32(0), jnp.int32(0)
    for b, key in enumerate(keys):
        hit = key == wanted
        first = jnp.where(jnp.logical_and(hit, count == 0), b, first)
        second = jnp.where(jnp.logical_and(hit, count == 1), b, second)
        count = count + hit.astype(jnp.int32)
    return first, second


def shared_rows(lvl, levels):
    return 16 * min(max(round(6 * (lvl + 2) / (levels + 2)), 1), 5)


def kernel(n, levels, spots_in, parents_in, flags_in, vort_in, shift_in, shrink_in, grow_in, out,
           spots, parent_slot, flags, field, shrink, grow,
           rows, patch, whole0, whole1, whole2, whole3, masks,
           send0, send1, send2, send3, got0, got1, got2, got3,
           small, ghost, relay, got_ghost,
           edge, edge_low, edge_high, below, above, halo_low, halo_high,
           tab, near_tabs, fine_tabs, near_local, fine_local, line, place, line2, octants,
           pick, pick_ghost,
           in_sem, index_sem, table_sem, halo_s, halo_r, near_s, near_r, down_s, down_r,
           block_s, block_r, ghost_s, ghost_r, relay_s, relay_r, direct_s, direct_r, plane_ready):
    me = lax.axis_index("blk")
    lvl = lax.axis_index("lvl")
    blocks = out.shape[1]
    spread = EDGE * LANE_TILES * blocks
    pitch = (LANE_TILES + 1) * blocks
    coarse_level = jnp.maximum(lvl - 1, 0)
    fine_level = jnp.minimum(lvl + 1, levels - 1)
    pieces = [(x1 - x0) * LANE_TILES for x0, x1 in PARTS]
    wholes = (whole0, whole1, whole2, whole3)
    sends, gots = (send0, send1, send2, send3), (got0, got1, got2, got3)
    after = device(lax.rem(me + 1, n), lvl)
    before = device(lax.rem(me + n - 1, n), lvl)
    below_level = device(me, coarse_level)
    has_coarse, has_fine = lvl > 0, lvl < levels - 1
    not_first, not_last = me > 0, me < n - 1

    others = range(1, n)
    partners = [lax.rem(me + k, n) for k in range(n)]
    sources = [lax.rem(me + n - k, n) for k in range(n)]

    barrier = pltpu.get_barrier_semaphore()

    def greet(blk, level):
        pl.semaphore_signal(barrier, inc=1, device_id=device(blk, level), device_id_type=MESH)

    for k in others:
        greet(partners[k], lvl)

    @pl.when(has_fine)
    def _():
        greet(me, fine_level)

    index_loads = [
        pltpu.make_async_copy(src, dst, index_sem.at[i])
        for i, (src, dst) in enumerate(((spots_in, spots), (parents_in, parent_slot), (flags_in, flags)))
    ]
    loads = []
    for i, (lo, hi) in enumerate(PIECES):
        part = pl.ds(lo, hi - lo)
        loads.append((
            pltpu.make_async_copy(shift_in.at[:, part], field.at[3, :, part], in_sem.at[2 * i]),
            pltpu.make_async_copy(vort_in.at[:, :, part], field.at[pl.ds(0, 3), :, part], in_sem.at[2 * i + 1]),
        ))
    constants = (
        pltpu.make_async_copy(shrink_in, shrink, table_sem.at[0]),
        pltpu.make_async_copy(grow_in, grow, table_sem.at[1]),
    )
    for copy in loads[0]:
        copy.start()
    for copy in index_loads:
        copy.start()
    for copy in loads[1] + loads[2]:
        copy.start()
    for copy in constants:
        copy.start()

    sublane = lax.broadcasted_iota(jnp.int32, (blocks, 128), 0)
    lane = lax.broadcasted_iota(jnp.int32, (1, 128), 1)

    def tile(f, x, j):
        at = pl.multiple_of(x * PLANE + j * 128, 128)
        return field[f, :, pl.ds(at, 128)].astype(jnp.float32)

    def source_tile(f, x, j):
        if x < 0:
            edge_row = halo_low[pl.ds(f * 16 + (x + 2) * LANE_TILES + j, 1), :]
            return jnp.where(sublane == 0, edge_row, pltpu.roll(tile(f, x + EDGE, j), 1, 0))
        if x >= EDGE:
            edge_row = halo_high[pl.ds(f * 16 + (x - EDGE) * LANE_TILES + j, 1), :]
            return jnp.where(sublane == blocks - 1, edge_row, pltpu.roll(tile(f, x - EDGE, j), blocks - 1, 0))
        return tile(f, x, j)

    def remesh(part):
        (x0, x1), piece = PARTS[part], pieces[part]

        def chunk(j, carry):
            sums = [{}, {}, {}]
            for x in range(x0 - 2, x1 + 2):
                weights = tap_weights(source_tile(3, x, j))
                for c in range(3):
                    value = source_tile(c, x, j)
                    for offset in range(-2, 3):
                        to = x + offset
                        if x0 <= to < x1:
                            term = value * weights[offset]
                            sums[c][to] = sums[c][to] + term if to in sums[c] else term
                    if x0 <= x - 2:
                        at = c * spread + ((x - 2) * LANE_TILES + j) * blocks
                        rows[pl.ds(pl.multiple_of(at, blocks), blocks), :] = sums[c].pop(x - 2)
            return carry

        lax.fori_loop(0, LANE_TILES, chunk, 0)
        for b in range(blocks):
            for c in range(3):
                at = c * spread + x0 * LANE_TILES * blocks + b
                wholes[part][b, c * piece:(c + 1) * piece, :] = rows[
                    pl.ds(at, piece, stride=blocks), :
                ].astype(jnp.bfloat16)

    def pack(part):
        def one(to, carry):
            for s in range(CAP):
                sends[part][to, s] = wholes[part][pick[CAP * to + s]]
            return carry

        lax.fori_loop(0, n, one, 0)

    def keep(part):
        for s in range(CAP):
            gots[part][CAP * me + s] = wholes[part][pick[CAP * me + s]]

    def block_copy(part, to):
        return remote(sends[part].at[to], gots[part].at[pl.ds(CAP * me, CAP)],
                      block_s.at[part, to], block_r.at[part, me], device(to, lvl))

    def block_arrival(part, source):
        return remote(sends[part].at[me], gots[part].at[pl.ds(CAP * source, CAP)],
                      block_s.at[part, source], block_r.at[part, source], before)

    def send_blocks(part):
        for k in others:
            block_copy(part, partners[k]).start()

    def near(k):
        return remote(tab, near_tabs.at[me], near_s.at[k], near_r.at[k], device(partners[k], lvl))

    def near_arrival(k):
        return remote(tab, near_tabs.at[sources[k]], near_s.at[k], near_r.at[k], before)

    def down():
        return remote(near_tabs, fine_tabs, down_s, down_r, below_level)

    def ghost_copy(k, size):
        part = pl.ds(0, size)
        return remote(ghost.at[partners[k], :, part], relay.at[pl.ds(CAP * me, CAP), part],
                      ghost_s.at[k], ghost_r.at[k], device(partners[k], lvl))

    def ghost_arrival(k, size):
        part = pl.ds(0, size)
        return remote(ghost.at[me, :, part], relay.at[pl.ds(CAP * sources[k], CAP), part],
                      ghost_s.at[k], ghost_r.at[k], before)

    def relay_copy(k, size):
        pair, part = pl.ds(CAP * sources[k], CAP), pl.ds(0, size)
        origin = ghost.at[me, :, part] if k == 0 else relay.at[pair, part]
        return remote(origin, got_ghost.at[pair, part], relay_s.at[k], relay_r.at[k], below_level)

    def direct_copy(k, size):
        part = pl.ds(size, 96 - size)
        return remote(ghost.at[partners[k], :, part], got_ghost.at[pl.ds(CAP * me, CAP), part],
                      direct_s.at[k], direct_r.at[k], device(partners[k], coarse_level))

    def direct_arrival(k, size):
        part = pl.ds(size, 96 - size)
        return remote(ghost.at[me, :, part], got_ghost.at[pl.ds(CAP * sources[k], CAP), part],
                      direct_s.at[k], direct_r.at[k], before)

    def on_level(shift, action):
        for level in range(1, levels):
            pl.when(lvl == level - shift)(functools.partial(action, shared_rows(level, levels)))

    def high(target):
        return remote(edge_high, below, halo_s.at[0], halo_r.at[0], target)

    def low(target):
        return remote(edge_low, above, halo_s.at[1], halo_r.at[1], target)

    for copy in index_loads:
        copy.wait()
    head = jnp.zeros((1, 128), jnp.int32)
    for part, ref in enumerate((spots, parent_slot, flags)):
        for b in range(blocks):
            head = jnp.where(lane == part * blocks + b, ref[0, b], head)
    tab[...] = head
    near_tabs[me] = head
    owners = [split(spots[0, b], blocks)[0] for b in range(blocks)]

    def choose(to, carry):
        first, second = picks(owners, to)
        pick[CAP * to] = first
        pick[CAP * to + 1] = second
        return carry

    lax.fori_loop(0, n, choose, 0)

    for copy in loads[0]:
        copy.wait()
    remesh(0)
    pack(0)
    for copy in loads[1] + loads[2]:
        copy.wait()

    def edges(j, carry):
        for f in range(4):
            for p in range(2):
                at = f * 16 + p * LANE_TILES + j
                edge[pl.ds(at, 1), :] = tile(f, p, j)[0:1, :]
                edge[pl.ds(64 + at, 1), :] = tile(f, EDGE - 2 + p, j)[blocks - 1:blocks, :]
        return carry

    lax.fori_loop(0, LANE_TILES, edges, 0)
    edge_low[...] = edge[0:64, :].astype(jnp.bfloat16)
    edge_high[...] = edge[64:128, :].astype(jnp.bfloat16)

    pl.semaphore_wait(barrier, n - 1 + has_coarse.astype(jnp.int32))

    send_blocks(0)

    @pl.when(not_last)
    def _():
        high(after).start()

    @pl.when(not_first)
    def _():
        low(before).start()

    for k in others:
        near(k).start()
    keep(0)
    remesh(1)
    pack(1)
    keep(1)
    send_blocks(1)

    @pl.when(not_last)
    def _():
        low(after).wait_recv()

    @pl.when(not_first)
    def _():
        high(before).wait_recv()

    halo_low[...] = jnp.where(not_first, below[...].astype(jnp.float32), 0.0)
    halo_high[...] = jnp.where(not_last, above[...].astype(jnp.float32), 0.0)
    for part in (2, 3):
        remesh(part)
        pack(part)
        keep(part)

    for k in others:
        near_arrival(k).wait_recv()

    @pl.when(has_coarse)
    def _():
        down().start()

    fetch_near = pltpu.make_async_copy(near_tabs, near_local, table_sem.at[2])
    fetch_near.start()
    fetch_near.wait()
    for copy in constants:
        copy.wait()

    @pl.when(has_coarse)
    def _():
        parents = []
        for b in range(blocks):
            home, spot = split(spots[0, b], blocks)
            parents.append(split(near_local[home, 0, blocks + spot], 8 * blocks)[0])

        def choose_ghost(to, carry):
            first, second = picks(parents, to)
            pick_ghost[CAP * to] = first
            pick_ghost[CAP * to + 1] = second
            return carry

        lax.fori_loop(0, n, choose_ghost, 0)

        def restrict(b, carry):
            columns = []
            for half in range(2):
                for dx in range(2):
                    for odd in range(2):
                        parts = []
                        for c in range(3):
                            for jj in range(4):
                                x, j = half * 16 + dx, 2 * jj + odd
                                at = c * spread + (x * LANE_TILES + j) * blocks + b
                                parts.append(rows[pl.ds(at, 8, stride=2 * LANE_TILES * blocks), :])
                        columns.append(jnp.concatenate(parts, axis=0).astype(jnp.bfloat16))
            wide = jnp.concatenate(columns, axis=1)
            small[b] = jnp.dot(wide, shrink[...], preferred_element_type=jnp.float32).astype(jnp.bfloat16)
            return carry

        lax.fori_loop(0, blocks, restrict, 0)

        def pack_ghost(to, carry):
            for s in range(CAP):
                ghost[to, s] = small[pick_ghost[CAP * to + s]]
            return carry

        lax.fori_loop(0, n, pack_ghost, 0)

    def settle_places(source, places):
        count = jnp.int32(0)
        for b in range(blocks):
            owner, spot = split(near_local[source, 0, b], blocks)
            mine = owner == me
            slot = CAP * source + jnp.minimum(count, CAP - 1)
            places = jnp.where(lane == jnp.where(mine, spot, -1), slot, places)
            count = count + mine.astype(jnp.int32)
        return places

    line[...] = lax.fori_loop(0, n, settle_places, jnp.zeros((1, 128), jnp.int32))
    def share(size):
        for k in others:
            ghost_copy(k, size).start()
        relay_copy(0, size).start()

    on_level(0, share)
    for part in (2, 3):
        send_blocks(part)

    @pl.when(has_fine)
    def _():
        down().wait_recv()
        pl.semaphore_signal(plane_ready, inc=1, device_id=device(me, fine_level), device_id_type=MESH)
        fetch_fine = pltpu.make_async_copy(fine_tabs, fine_local, table_sem.at[4])
        fetch_fine.start()
        fetch_fine.wait()

    @pl.when(has_coarse)
    def _():
        pl.semaphore_wait(plane_ready, 1)

    def rest(size):
        for k in range(n):
            direct_copy(k, size).start()

    on_level(0, rest)
    empty = CAP * n

    def settle_octants(source, codes):
        count = jnp.int32(0)
        for b in range(blocks):
            home, spot = split(fine_local[source, 0, b], blocks)
            owner, code = split(fine_local[home, 0, blocks + spot], 8 * blocks)
            mine = owner == me
            hit = jnp.logical_and(mine, fine_local[home, 0, 2 * blocks + spot] == 1)
            slot = CAP * source + jnp.minimum(count, CAP - 1)
            codes = jnp.where(lane == jnp.where(hit, code, -1), slot, codes)
            count = count + mine.astype(jnp.int32)
        return codes

    rounds = jnp.where(has_fine, n, 0)
    line2[...] = lax.fori_loop(0, rounds, settle_octants, jnp.full((1, 128), empty, jnp.int32))
    got_ghost[empty] = jnp.zeros(got_ghost.shape[1:], jnp.bfloat16)
    fetch_place = pltpu.make_async_copy(line, place, table_sem.at[3])
    fetch_octants = pltpu.make_async_copy(line2, octants, table_sem.at[5])
    fetch_place.start()
    fetch_octants.start()
    fetch_place.wait()
    fetch_octants.wait()

    wide_lane = lax.broadcasted_iota(jnp.int32, (blocks, 128), 1)
    deep = lax.bitwise_and(wide_lane, 16) != 0
    for corner in range(4):
        mask = jnp.zeros((blocks, 128), jnp.int32)
        for q in range(blocks):
            near_half = (octants[0, q * 8 + corner * 2] < empty).astype(jnp.int32)
            far_half = (octants[0, q * 8 + corner * 2 + 1] < empty).astype(jnp.int32)
            mask = jnp.where(sublane == q, jnp.where(deep, far_half, near_half), mask)
        masks[corner] = mask

    def scatter(part):
        for k in others:
            block_arrival(part, sources[k]).wait_recv()

        piece = pieces[part]

        def one(q, carry):
            block = gots[part][place[0, q]].astype(jnp.float32)
            for c in range(3):
                at = c * spread + PARTS[part][0] * LANE_TILES * blocks + q
                rows[pl.ds(at, piece, stride=blocks), :] = block[c * piece:(c + 1) * piece, :]
            return carry

        lax.fori_loop(0, blocks, one, 0)

    def finish(part):
        def one(x, carry):
            flagged = [masks[2 * lax.div(x, 16) + oy] != 0 for oy in range(2)]
            for c in range(3):
                for j in range(LANE_TILES):
                    at = pl.multiple_of(c * spread + (x * LANE_TILES + j) * blocks, blocks)
                    over = pl.multiple_of((c * EDGE + x) * pitch + j * blocks, blocks)
                    value = jnp.where(flagged[j // 4], patch[pl.ds(over, blocks), :], rows[pl.ds(at, blocks), :])
                    to = pl.multiple_of(x * PLANE + j * 128, 128)
                    out[c, :, pl.ds(to, 128)] = value.astype(jnp.bfloat16)
            return carry

        lax.fori_loop(*PARTS[part], one, 0)

    scatter(0)
    scatter(1)

    def forward(size):
        for k in others:
            ghost_arrival(k, size).wait_recv()
            relay_copy(k, size).start()

    def gather(size):
        for k in range(n):
            relay_copy(k, size).wait_recv()
            direct_arrival(k, size).wait_recv()

    on_level(0, forward)
    scatter(2)
    on_level(1, gather)

    @pl.when(has_fine)
    def _():
        def expand(q, carry):
            pairs = []
            for corner in range(4):
                at = q * 8 + corner * 2
                pairs.append(jnp.concatenate([got_ghost[octants[0, at]], got_ghost[octants[0, at + 1]]], axis=1))
            full = jnp.dot(jnp.concatenate(pairs, axis=0), grow[...], preferred_element_type=jnp.float32)
            for corner in range(4):
                for c in range(3):
                    for jj in range(4):
                        for half in range(2):
                            x, j = corner // 2 * 16 + half * 8, corner % 2 * 4 + jj
                            to = (c * EDGE + x) * pitch + j * blocks + q
                            at = (corner * 12 + c * 4 + jj) * 8
                            patch[pl.ds(to, 8, stride=pitch), :] = full[at:at + 8, half * 128:(half + 1) * 128]
            return carry

        lax.fori_loop(0, blocks, expand, 0)

    for part in (0, 1, 2):
        finish(part)
    scatter(3)
    finish(3)

    @pl.when(not_last)
    def _():
        high(after).wait_send()

    @pl.when(not_first)
    def _():
        low(before).wait_send()

    for k in others:
        near(k).wait_send()
        for part in range(len(PARTS)):
            block_copy(part, partners[k]).wait_send()

    @pl.when(has_coarse)
    def _():
        down().wait_send()

    def drain(size):
        for k in others:
            ghost_copy(k, size).wait_send()
        for k in range(n):
            relay_copy(k, size).wait_send()
            direct_copy(k, size).wait_send()

    on_level(0, drain)


def selection_tables():
    k = np.arange(1024)
    half, dx, odd, y, z = k // 512, k // 256 % 2, k // 128 % 2, k % 128 // 32, k % 32
    target = half * 64 + (2 * odd + y // 2) * 16 + z // 2
    shrink = np.where(target[:, None] == np.arange(128)[None, :], 0.125, 0.0)
    k = np.arange(256)
    oz, half, y, z = k // 128, k % 128 // 64, k % 64 // 16, k % 16
    target = half * 128 + y * 32 + oz * 16 + z
    grow = np.where(target[:, None] == np.arange(256)[None, :], 1.0, 0.0)
    return shrink, grow


def body(n, levels, vorticity, shift_field, new_index, parent_slot, flags):
    blocks, cells = vorticity.shape[2:]
    vort, shift = vorticity[0], shift_field[0]
    hbm = pl.BlockSpec(memory_space=pltpu.HBM)
    vmem = pl.BlockSpec(memory_space=pltpu.VMEM)
    bf16, f32, i32 = jnp.bfloat16, jnp.float32, jnp.int32
    dma, vm, smem = pltpu.SemaphoreType.DMA, pltpu.VMEM, pltpu.SMEM
    spread = EDGE * LANE_TILES * blocks
    pieces = [3 * (x1 - x0) * LANE_TILES for x0, x1 in PARTS]
    parts = len(PARTS)
    shrink, grow = selection_tables()
    out = pl.pallas_call(
        functools.partial(kernel, n, levels),
        out_shape=jax.ShapeDtypeStruct((3, blocks, cells), bf16),
        in_specs=[hbm] * 7,
        out_specs=vmem,
        scratch_shapes=[
            smem((1, blocks), i32), smem((1, blocks), i32), smem((1, blocks), i32),
            vm((4, blocks, cells), bf16), vm(shrink.shape, bf16), vm(grow.shape, bf16),
            vm((3 * spread, 128), f32), vm((3 * EDGE * (LANE_TILES + 1) * blocks, 128), f32),
            *[vm((blocks, piece, 128), bf16) for piece in pieces], vm((4, blocks, 128), i32),
            *[vm((n, CAP, piece, 128), bf16) for piece in pieces],
            *[vm((n * CAP, piece, 128), bf16) for piece in pieces],
            vm((blocks, 96, 128), bf16), vm((n, CAP, 96, 128), bf16), vm((n * CAP, 96, 128), bf16),
            vm((n * CAP + 1, 96, 128), bf16),
            vm((128, 128), f32), vm((64, 128), bf16), vm((64, 128), bf16),
            vm((64, 128), bf16), vm((64, 128), bf16), vm((64, 128), f32), vm((64, 128), f32),
            vm((1, 128), i32), vm((n, 1, 128), i32), vm((n, 1, 128), i32),
            smem((n, 1, 128), i32), smem((n, 1, 128), i32),
            vm((1, 128), i32), smem((1, 128), i32), vm((1, 128), i32), smem((1, 128), i32),
            smem((CAP * n,), i32), smem((CAP * n,), i32),
            dma((6,)), dma((3,)), dma((6,)), dma((2,)), dma((2,)), dma((n,)), dma((n,)), dma, dma,
            dma((parts, n)), dma((parts, n)), dma((n,)), dma((n,)), dma((n,)), dma((n,)), dma((n,)), dma((n,)),
            pltpu.SemaphoreType.REGULAR,
        ],
        compiler_params=pltpu.CompilerParams(
            collective_id=0, has_side_effects=True, vmem_limit_bytes=VMEM_LIMIT
        ),
        name="move",
    )(*[
        pltpu.with_memory_space_constraint(x, pltpu.HBM)
        for x in (new_index, parent_slot, flags, vort, shift, jnp.asarray(shrink, bf16), jnp.asarray(grow, bf16))
    ])
    return out[None]


def solution(mesh):
    placed = (
        P("lvl", None, "blk", None),
        P("lvl", "blk", None),
        P("lvl", "blk"),
        P("lvl", "blk"),
        P("lvl", "blk"),
    )
    step = functools.partial(body, mesh.shape["blk"], mesh.shape["lvl"])
    return jax.shard_map(
        step, mesh=mesh, in_specs=placed, out_specs=P("lvl", None, "blk", None), check_vma=False
    )
```

```python
import functools

import jax
import jax.numpy as jnp
import numpy as np
from jax import lax
from jax.experimental import pallas as pl
from jax.experimental.pallas import tpu as pltpu
from jax.sharding import PartitionSpec as P

MESH = pl.DeviceIdType.MESH
EDGE = 32
PLANE = EDGE * EDGE
LANE_TILES = PLANE // 128
CAP = 2
PARTS = ((4, 8), (8, 22), (22, 32), (0, 4))
VMEM_LIMIT = 44 * 1024 * 1024
PIECES = ((2 * PLANE, 10 * PLANE), (10 * PLANE, 32 * PLANE), (0, 2 * PLANE))


def device(blk, lvl):
    return {"blk": blk, "lvl": lvl}


def remote(src, dst, send, recv, target):
    return pltpu.make_async_remote_copy(
        src_ref=src, dst_ref=dst, send_sem=send, recv_sem=recv, device_id=target, device_id_type=MESH
    )


def tap_weights(shifts):
    size = jnp.abs(shifts)
    rest = 1.0 - size
    size2 = size * size
    rest2 = rest * rest
    middle = 1.0 + size2 * (1.5 * size - 2.5)
    ahead = 1.0 + rest2 * (1.5 * rest - 2.5)
    behind = -0.5 * rest2 * size
    far = -0.5 * size2 * rest
    up = shifts >= 0.0
    return {
        -2: jnp.where(up, 0.0, far),
        -1: jnp.where(up, behind, ahead),
        0: middle,
        1: jnp.where(up, ahead, behind),
        2: jnp.where(up, far, 0.0),
    }


def split(value, size):
    if size & (size - 1) == 0:
        return lax.shift_right_logical(value, size.bit_length() - 1), lax.bitwise_and(value, size - 1)
    return lax.div(value, size), lax.rem(value, size)


def picks(keys, wanted):
    count, first, second = jnp.int32(0), jnp.int32(0), jnp.int32(0)
    for b, key in enumerate(keys):
        hit = key == wanted
        first = jnp.where(jnp.logical_and(hit, count == 0), b, first)
        second = jnp.where(jnp.logical_and(hit, count == 1), b, second)
        count = count + hit.astype(jnp.int32)
    return first, second


def shared_rows(lvl, levels):
    return 16 * min(max(round(6 * (lvl + 2) / (levels + 2)), 1), 5)


def kernel(n, levels, spots_in, parents_in, flags_in, vort_in, shift_in, shrink_in, grow_in, out,
           spots, parent_slot, flags, field, shrink, grow,
           rows, patch, whole0, whole1, whole2, whole3, masks,
           send0, send1, send2, send3, got0, got1, got2, got3,
           small, ghost, relay, got_ghost,
           edge, edge_low, edge_high, below, above, halo_low, halo_high,
           tab, near_tabs, fine_tabs, near_local, fine_local, line, place, line2, octants,
           pick, pick_ghost,
           in_sem, index_sem, table_sem, halo_s, halo_r, near_s, near_r, down_s, down_r,
           block_s, block_r, ghost_s, ghost_r, relay_s, relay_r, direct_s, direct_r, plane_ready):
    me = lax.axis_index("blk")
    lvl = lax.axis_index("lvl")
    blocks = out.shape[1]
    spread = EDGE * LANE_TILES * blocks
    pitch = (LANE_TILES + 1) * blocks
    coarse_level = jnp.maximum(lvl - 1, 0)
    fine_level = jnp.minimum(lvl + 1, levels - 1)
    pieces = [(x1 - x0) * LANE_TILES for x0, x1 in PARTS]
    wholes = (whole0, whole1, whole2, whole3)
    sends, gots = (send0, send1, send2, send3), (got0, got1, got2, got3)
    after = device(lax.rem(me + 1, n), lvl)
    before = device(lax.rem(me + n - 1, n), lvl)
    below_level = device(me, coarse_level)
    has_coarse, has_fine = lvl > 0, lvl < levels - 1
    not_first, not_last = me > 0, me < n - 1

    others = range(1, n)
    partners = [lax.rem(me + k, n) for k in range(n)]
    sources = [lax.rem(me + n - k, n) for k in range(n)]

    barrier = pltpu.get_barrier_semaphore()

    def greet(blk, level):
        pl.semaphore_signal(barrier, inc=1, device_id=device(blk, level), device_id_type=MESH)

    for k in others:
        greet(partners[k], lvl)

    @pl.when(has_fine)
    def _():
        greet(me, fine_level)

    index_loads = [
        pltpu.make_async_copy(src, dst, index_sem.at[i])
        for i, (src, dst) in enumerate(((spots_in, spots), (parents_in, parent_slot), (flags_in, flags)))
    ]
    loads = []
    for i, (lo, hi) in enumerate(PIECES):
        part = pl.ds(lo, hi - lo)
        loads.append((
            pltpu.make_async_copy(shift_in.at[:, part], field.at[3, :, part], in_sem.at[2 * i]),
            pltpu.make_async_copy(vort_in.at[:, :, part], field.at[pl.ds(0, 3), :, part], in_sem.at[2 * i + 1]),
        ))
    constants = (
        pltpu.make_async_copy(shrink_in, shrink, table_sem.at[0]),
        pltpu.make_async_copy(grow_in, grow, table_sem.at[1]),
    )
    for copy in loads[0]:
        copy.start()
    for copy in index_loads:
        copy.start()
    for copy in loads[1] + loads[2]:
        copy.start()
    for copy in constants:
        copy.start()

    sublane = lax.broadcasted_iota(jnp.int32, (blocks, 128), 0)
    lane = lax.broadcasted_iota(jnp.int32, (1, 128), 1)

    def tile(f, x, j):
        at = pl.multiple_of(x * PLANE + j * 128, 128)
        return field[f, :, pl.ds(at, 128)].astype(jnp.float32)

    def source_tile(f, x, j):
        if x < 0:
            edge_row = halo_low[pl.ds(f * 16 + (x + 2) * LANE_TILES + j, 1), :]
            return jnp.where(sublane == 0, edge_row, pltpu.roll(tile(f, x + EDGE, j), 1, 0))
        if x >= EDGE:
            edge_row = halo_high[pl.ds(f * 16 + (x - EDGE) * LANE_TILES + j, 1), :]
            return jnp.where(sublane == blocks - 1, edge_row, pltpu.roll(tile(f, x - EDGE, j), blocks - 1, 0))
        return tile(f, x, j)

    def remesh(part):
        (x0, x1), piece = PARTS[part], pieces[part]

        def chunk(j, carry):
            sums = [{}, {}, {}]
            for x in range(x0 - 2, x1 + 2):
                weights = tap_weights(source_tile(3, x, j))
                for c in range(3):
                    value = source_tile(c, x, j)
                    for offset in range(-2, 3):
                        to = x + offset
                        if x0 <= to < x1:
                            term = value * weights[offset]
                            sums[c][to] = sums[c][to] + term if to in sums[c] else term
                    if x0 <= x - 2:
                        at = c * spread + ((x - 2) * LANE_TILES + j) * blocks
                        rows[pl.ds(pl.multiple_of(at, blocks), blocks), :] = sums[c].pop(x - 2)
            return carry

        lax.fori_loop(0, LANE_TILES, chunk, 0)
        for b in range(blocks):
            for c in range(3):
                at = c * spread + x0 * LANE_TILES * blocks + b
                wholes[part][b, c * piece:(c + 1) * piece, :] = rows[
                    pl.ds(at, piece, stride=blocks), :
                ].astype(jnp.bfloat16)

    def pack(part):
        def one(to, carry):
            for s in range(CAP):
                sends[part][to, s] = wholes[part][pick[CAP * to + s]]
            return carry

        lax.fori_loop(0, n, one, 0)

    def keep(part):
        for s in range(CAP):
            gots[part][CAP * me + s] = wholes[part][pick[CAP * me + s]]

    def block_copy(part, to):
        return remote(sends[part].at[to], gots[part].at[pl.ds(CAP * me, CAP)],
                      block_s.at[part, to], block_r.at[part, me], device(to, lvl))

    def block_arrival(part, source):
        return remote(sends[part].at[me], gots[part].at[pl.ds(CAP * source, CAP)],
                      block_s.at[part, source], block_r.at[part, source], before)

    def send_blocks(part):
        for k in others:
            block_copy(part, partners[k]).start()

    def near(k):
        return remote(tab, near_tabs.at[me], near_s.at[k], near_r.at[k], device(partners[k], lvl))

    def near_arrival(k):
        return remote(tab, near_tabs.at[sources[k]], near_s.at[k], near_r.at[k], before)

    def down():
        return remote(near_tabs, fine_tabs, down_s, down_r, below_level)

    def ghost_copy(k, size):
        part = pl.ds(0, size)
        return remote(ghost.at[partners[k], :, part], relay.at[pl.ds(CAP * me, CAP), part],
                      ghost_s.at[k], ghost_r.at[k], device(partners[k], lvl))

    def ghost_arrival(k, size):
        part = pl.ds(0, size)
        return remote(ghost.at[me, :, part], relay.at[pl.ds(CAP * sources[k], CAP), part],
                      ghost_s.at[k], ghost_r.at[k], before)

    def relay_copy(k, size):
        pair, part = pl.ds(CAP * sources[k], CAP), pl.ds(0, size)
        origin = ghost.at[me, :, part] if k == 0 else relay.at[pair, part]
        return remote(origin, got_ghost.at[pair, part], relay_s.at[k], relay_r.at[k], below_level)

    def direct_copy(k, size):
        part = pl.ds(size, 96 - size)
        return remote(ghost.at[partners[k], :, part], got_ghost.at[pl.ds(CAP * me, CAP), part],
                      direct_s.at[k], direct_r.at[k], device(partners[k], coarse_level))

    def direct_arrival(k, size):
        part = pl.ds(size, 96 - size)
        return remote(ghost.at[me, :, part], got_ghost.at[pl.ds(CAP * sources[k], CAP), part],
                      direct_s.at[k], direct_r.at[k], before)

    def on_level(shift, action):
        for level in range(1, levels):
            pl.when(lvl == level - shift)(functools.partial(action, shared_rows(level, levels)))

    def high(target):
        return remote(edge_high, below, halo_s.at[0], halo_r.at[0], target)

    def low(target):
        return remote(edge_low, above, halo_s.at[1], halo_r.at[1], target)

    for copy in index_loads:
        copy.wait()
    head = jnp.zeros((1, 128), jnp.int32)
    for part, ref in enumerate((spots, parent_slot, flags)):
        for b in range(blocks):
            head = jnp.where(lane == part * blocks + b, ref[0, b], head)
    tab[...] = head
    near_tabs[me] = head
    owners = [split(spots[0, b], blocks)[0] for b in range(blocks)]

    def choose(to, carry):
        first, second = picks(owners, to)
        pick[CAP * to] = first
        pick[CAP * to + 1] = second
        return carry

    lax.fori_loop(0, n, choose, 0)

    for copy in loads[0]:
        copy.wait()
    remesh(0)
    pack(0)
    for copy in loads[1] + loads[2]:
        copy.wait()

    def edges(j, carry):
        for f in range(4):
            for p in range(2):
                at = f * 16 + p * LANE_TILES + j
                edge[pl.ds(at, 1), :] = tile(f, p, j)[0:1, :]
                edge[pl.ds(64 + at, 1), :] = tile(f, EDGE - 2 + p, j)[blocks - 1:blocks, :]
        return carry

    lax.fori_loop(0, LANE_TILES, edges, 0)
    edge_low[...] = edge[0:64, :].astype(jnp.bfloat16)
    edge_high[...] = edge[64:128, :].astype(jnp.bfloat16)

    pl.semaphore_wait(barrier, n - 1 + has_coarse.astype(jnp.int32))

    send_blocks(0)

    @pl.when(not_last)
    def _():
        high(after).start()

    @pl.when(not_first)
    def _():
        low(before).start()

    for k in others:
        near(k).start()
    keep(0)
    remesh(1)
    pack(1)
    keep(1)
    send_blocks(1)

    @pl.when(not_last)
    def _():
        low(after).wait_recv()

    @pl.when(not_first)
    def _():
        high(before).wait_recv()

    halo_low[...] = jnp.where(not_first, below[...].astype(jnp.float32), 0.0)
    halo_high[...] = jnp.where(not_last, above[...].astype(jnp.float32), 0.0)
    for part in (2, 3):
        remesh(part)
        pack(part)
        keep(part)

    for k in others:
        near_arrival(k).wait_recv()

    @pl.when(has_coarse)
    def _():
        down().start()

    fetch_near = pltpu.make_async_copy(near_tabs, near_local, table_sem.at[2])
    fetch_near.start()
    fetch_near.wait()
    for copy in constants:
        copy.wait()

    @pl.when(has_coarse)
    def _():
        parents = []
        for b in range(blocks):
            home, spot = split(spots[0, b], blocks)
            parents.append(split(near_local[home, 0, blocks + spot], 8 * blocks)[0])

        def choose_ghost(to, carry):
            first, second = picks(parents, to)
            pick_ghost[CAP * to] = first
            pick_ghost[CAP * to + 1] = second
            return carry

        lax.fori_loop(0, n, choose_ghost, 0)

        def restrict(b, carry):
            columns = []
            for half in range(2):
                for dx in range(2):
                    for odd in range(2):
                        parts = []
                        for c in range(3):
                            for jj in range(4):
                                x, j = half * 16 + dx, 2 * jj + odd
                                at = c * spread + (x * LANE_TILES + j) * blocks + b
                                parts.append(rows[pl.ds(at, 8, stride=2 * LANE_TILES * blocks), :])
                        columns.append(jnp.concatenate(parts, axis=0).astype(jnp.bfloat16))
            wide = jnp.concatenate(columns, axis=1)
            small[b] = jnp.dot(wide, shrink[...], preferred_element_type=jnp.float32).astype(jnp.bfloat16)
            return carry

        lax.fori_loop(0, blocks, restrict, 0)

        def pack_ghost(to, carry):
            for s in range(CAP):
                ghost[to, s] = small[pick_ghost[CAP * to + s]]
            return carry

        lax.fori_loop(0, n, pack_ghost, 0)

    def settle_places(source, places):
        count = jnp.int32(0)
        for b in range(blocks):
            owner, spot = split(near_local[source, 0, b], blocks)
            mine = owner == me
            slot = CAP * source + jnp.minimum(count, CAP - 1)
            places = jnp.where(lane == jnp.where(mine, spot, -1), slot, places)
            count = count + mine.astype(jnp.int32)
        return places

    line[...] = lax.fori_loop(0, n, settle_places, jnp.zeros((1, 128), jnp.int32))
    def share(size):
        for k in others:
            ghost_copy(k, size).start()
        relay_copy(0, size).start()

    on_level(0, share)
    for part in (2, 3):
        send_blocks(part)

    @pl.when(has_fine)
    def _():
        down().wait_recv()
        pl.semaphore_signal(plane_ready, inc=1, device_id=device(me, fine_level), device_id_type=MESH)
        fetch_fine = pltpu.make_async_copy(fine_tabs, fine_local, table_sem.at[4])
        fetch_fine.start()
        fetch_fine.wait()

    @pl.when(has_coarse)
    def _():
        pl.semaphore_wait(plane_ready, 1)

    def rest(size):
        for k in range(n):
            direct_copy(k, size).start()

    on_level(0, rest)
    empty = CAP * n

    def settle_octants(source, codes):
        count = jnp.int32(0)
        for b in range(blocks):
            home, spot = split(fine_local[source, 0, b], blocks)
            owner, code = split(fine_local[home, 0, blocks + spot], 8 * blocks)
            mine = owner == me
            hit = jnp.logical_and(mine, fine_local[home, 0, 2 * blocks + spot] == 1)
            slot = CAP * source + jnp.minimum(count, CAP - 1)
            codes = jnp.where(lane == jnp.where(hit, code, -1), slot, codes)
            count = count + mine.astype(jnp.int32)
        return codes

    rounds = jnp.where(has_fine, n, 0)
    line2[...] = lax.fori_loop(0, rounds, settle_octants, jnp.full((1, 128), empty, jnp.int32))
    got_ghost[empty] = jnp.zeros(got_ghost.shape[1:], jnp.bfloat16)
    fetch_place = pltpu.make_async_copy(line, place, table_sem.at[3])
    fetch_octants = pltpu.make_async_copy(line2, octants, table_sem.at[5])
    fetch_place.start()
    fetch_octants.start()
    fetch_place.wait()
    fetch_octants.wait()

    wide_lane = lax.broadcasted_iota(jnp.int32, (blocks, 128), 1)
    deep = lax.bitwise_and(wide_lane, 16) != 0
    for corner in range(4):
        mask = jnp.zeros((blocks, 128), jnp.int32)
        for q in range(blocks):
            near_half = (octants[0, q * 8 + corner * 2] < empty).astype(jnp.int32)
            far_half = (octants[0, q * 8 + corner * 2 + 1] < empty).astype(jnp.int32)
            mask = jnp.where(sublane == q, jnp.where(deep, far_half, near_half), mask)
        masks[corner] = mask

    def scatter(part):
        for k in others:
            block_arrival(part, sources[k]).wait_recv()

        piece = pieces[part]

        def one(q, carry):
            block = gots[part][place[0, q]].astype(jnp.float32)
            for c in range(3):
                at = c * spread + PARTS[part][0] * LANE_TILES * blocks + q
                rows[pl.ds(at, piece, stride=blocks), :] = block[c * piece:(c + 1) * piece, :]
            return carry

        lax.fori_loop(0, blocks, one, 0)

    def finish(part):
        def one(x, carry):
            flagged = [masks[2 * lax.div(x, 16) + oy] != 0 for oy in range(2)]
            for c in range(3):
                for j in range(LANE_TILES):
                    at = pl.multiple_of(c * spread + (x * LANE_TILES + j) * blocks, blocks)
                    over = pl.multiple_of((c * EDGE + x) * pitch + j * blocks, blocks)
                    value = jnp.where(flagged[j // 4], patch[pl.ds(over, blocks), :], rows[pl.ds(at, blocks), :])
                    to = pl.multiple_of(x * PLANE + j * 128, 128)
                    out[c, :, pl.ds(to, 128)] = value.astype(jnp.bfloat16)
            return carry

        lax.fori_loop(*PARTS[part], one, 0)

    scatter(0)
    scatter(1)

    def forward(size):
        for k in others:
            ghost_arrival(k, size).wait_recv()
            relay_copy(k, size).start()

    def gather(size):
        for k in range(n):
            relay_copy(k, size).wait_recv()
            direct_arrival(k, size).wait_recv()

    on_level(0, forward)
    scatter(2)
    on_level(1, gather)

    @pl.when(has_fine)
    def _():
        def expand(q, carry):
            pairs = []
            for corner in range(4):
                at = q * 8 + corner * 2
                pairs.append(jnp.concatenate([got_ghost[octants[0, at]], got_ghost[octants[0, at + 1]]], axis=1))
            full = jnp.dot(jnp.concatenate(pairs, axis=0), grow[...], preferred_element_type=jnp.float32)
            for corner in range(4):
                for c in range(3):
                    for jj in range(4):
                        for half in range(2):
                            x, j = corner // 2 * 16 + half * 8, corner % 2 * 4 + jj
                            to = (c * EDGE + x) * pitch + j * blocks + q
                            at = (corner * 12 + c * 4 + jj) * 8
                            patch[pl.ds(to, 8, stride=pitch), :] = full[at:at + 8, half * 128:(half + 1) * 128]
            return carry

        lax.fori_loop(0, blocks, expand, 0)

    for part in (0, 1, 2):
        finish(part)
    scatter(3)
    finish(3)

    @pl.when(not_last)
    def _():
        high(after).wait_send()

    @pl.when(not_first)
    def _():
        low(before).wait_send()

    for k in others:
        near(k).wait_send()
        for part in range(len(PARTS)):
            block_copy(part, partners[k]).wait_send()

    @pl.when(has_coarse)
    def _():
        down().wait_send()

    def drain(size):
        for k in others:
            ghost_copy(k, size).wait_send()
        for k in range(n):
            relay_copy(k, size).wait_send()
            direct_copy(k, size).wait_send()

    on_level(0, drain)


def selection_tables():
    k = np.arange(1024)
    half, dx, odd, y, z = k // 512, k // 256 % 2, k // 128 % 2, k % 128 // 32, k % 32
    target = half * 64 + (2 * odd + y // 2) * 16 + z // 2
    shrink = np.where(target[:, None] == np.arange(128)[None, :], 0.125, 0.0)
    k = np.arange(256)
    oz, half, y, z = k // 128, k % 128 // 64, k % 64 // 16, k % 16
    target = half * 128 + y * 32 + oz * 16 + z
    grow = np.where(target[:, None] == np.arange(256)[None, :], 1.0, 0.0)
    return shrink, grow


def body(n, levels, vorticity, shift_field, new_index, parent_slot, flags):
    blocks, cells = vorticity.shape[2:]
    vort, shift = vorticity[0], shift_field[0]
    hbm = pl.BlockSpec(memory_space=pltpu.HBM)
    vmem = pl.BlockSpec(memory_space=pltpu.VMEM)
    bf16, f32, i32 = jnp.bfloat16, jnp.float32, jnp.int32
    dma, vm, smem = pltpu.SemaphoreType.DMA, pltpu.VMEM, pltpu.SMEM
    spread = EDGE * LANE_TILES * blocks
    pieces = [3 * (x1 - x0) * LANE_TILES for x0, x1 in PARTS]
    parts = len(PARTS)
    shrink, grow = selection_tables()
    out = pl.pallas_call(
        functools.partial(kernel, n, levels),
        out_shape=jax.ShapeDtypeStruct((3, blocks, cells), bf16),
        in_specs=[hbm] * 7,
        out_specs=vmem,
        scratch_shapes=[
            smem((1, blocks), i32), smem((1, blocks), i32), smem((1, blocks), i32),
            vm((4, blocks, cells), bf16), vm(shrink.shape, bf16), vm(grow.shape, bf16),
            vm((3 * spread, 128), f32), vm((3 * EDGE * (LANE_TILES + 1) * blocks, 128), f32),
            *[vm((blocks, piece, 128), bf16) for piece in pieces], vm((4, blocks, 128), i32),
            *[vm((n, CAP, piece, 128), bf16) for piece in pieces],
            *[vm((n * CAP, piece, 128), bf16) for piece in pieces],
            vm((blocks, 96, 128), bf16), vm((n, CAP, 96, 128), bf16), vm((n * CAP, 96, 128), bf16),
            vm((n * CAP + 1, 96, 128), bf16),
            vm((128, 128), f32), vm((64, 128), bf16), vm((64, 128), bf16),
            vm((64, 128), bf16), vm((64, 128), bf16), vm((64, 128), f32), vm((64, 128), f32),
            vm((1, 128), i32), vm((n, 1, 128), i32), vm((n, 1, 128), i32),
            smem((n, 1, 128), i32), smem((n, 1, 128), i32),
            vm((1, 128), i32), smem((1, 128), i32), vm((1, 128), i32), smem((1, 128), i32),
            smem((CAP * n,), i32), smem((CAP * n,), i32),
            dma((6,)), dma((3,)), dma((6,)), dma((2,)), dma((2,)), dma((n,)), dma((n,)), dma, dma,
            dma((parts, n)), dma((parts, n)), dma((n,)), dma((n,)), dma((n,)), dma((n,)), dma((n,)), dma((n,)),
            pltpu.SemaphoreType.REGULAR,
        ],
        compiler_params=pltpu.CompilerParams(
            collective_id=0, has_side_effects=True, vmem_limit_bytes=VMEM_LIMIT
        ),
        name="move",
    )(*[
        pltpu.with_memory_space_constraint(x, pltpu.HBM)
        for x in (new_index, parent_slot, flags, vort, shift, jnp.asarray(shrink, bf16), jnp.asarray(grow, bf16))
    ])
    return out[None]


def solution(mesh):
    placed = (
        P("lvl", None, "blk", None),
        P("lvl", "blk", None),
        P("lvl", "blk"),
        P("lvl", "blk"),
        P("lvl", "blk"),
    )
    step = functools.partial(body, mesh.shape["blk"], mesh.shape["lvl"])
    return jax.shard_map(
        step, mesh=mesh, in_specs=placed, out_specs=P("lvl", None, "blk", None), check_vma=False
    )
```

```python
import functools

import jax
import jax.numpy as jnp
import numpy as np
from jax import lax
from jax.experimental import pallas as pl
from jax.experimental.pallas import tpu as pltpu
from jax.sharding import PartitionSpec as P

MESH = pl.DeviceIdType.MESH
EDGE = 32
PLANE = EDGE * EDGE
LANE_TILES = PLANE // 128
CAP = 2
PARTS = ((4, 8), (8, 22), (22, 32), (0, 4))
VMEM_LIMIT = 44 * 1024 * 1024
PIECES = ((2 * PLANE, 10 * PLANE), (10 * PLANE, 32 * PLANE), (0, 2 * PLANE))


def device(blk, lvl):
    return {"blk": blk, "lvl": lvl}


def remote(src, dst, send, recv, target):
    return pltpu.make_async_remote_copy(
        src_ref=src, dst_ref=dst, send_sem=send, recv_sem=recv, device_id=target, device_id_type=MESH
    )


def tap_weights(shifts):
    size = jnp.abs(shifts)
    rest = 1.0 - size
    size2 = size * size
    rest2 = rest * rest
    middle = 1.0 + size2 * (1.5 * size - 2.5)
    ahead = 1.0 + rest2 * (1.5 * rest - 2.5)
    behind = -0.5 * rest2 * size
    far = -0.5 * size2 * rest
    up = shifts >= 0.0
    return {
        -2: jnp.where(up, 0.0, far),
        -1: jnp.where(up, behind, ahead),
        0: middle,
        1: jnp.where(up, ahead, behind),
        2: jnp.where(up, far, 0.0),
    }


def split(value, size):
    if size & (size - 1) == 0:
        return lax.shift_right_logical(value, size.bit_length() - 1), lax.bitwise_and(value, size - 1)
    return lax.div(value, size), lax.rem(value, size)


def picks(keys, wanted):
    count, first, second = jnp.int32(0), jnp.int32(0), jnp.int32(0)
    for b, key in enumerate(keys):
        hit = key == wanted
        first = jnp.where(jnp.logical_and(hit, count == 0), b, first)
        second = jnp.where(jnp.logical_and(hit, count == 1), b, second)
        count = count + hit.astype(jnp.int32)
    return first, second


def shared_rows(lvl, levels):
    return 16 * min(max(round(6 * (lvl + 2) / (levels + 2)), 1), 5)


def kernel(n, levels, spots_in, parents_in, flags_in, vort_in, shift_in, shrink_in, grow_in, out,
           spots, parent_slot, flags, field, shrink, grow,
           rows, patch, whole0, whole1, whole2, whole3, masks,
           send0, send1, send2, send3, got0, got1, got2, got3,
           small, ghost, relay, got_ghost,
           edge, edge_low, edge_high, below, above, halo_low, halo_high,
           tab, near_tabs, fine_tabs, near_local, fine_local, line, place, line2, octants,
           pick, pick_ghost,
           in_sem, index_sem, table_sem, halo_s, halo_r, near_s, near_r, down_s, down_r,
           block_s, block_r, ghost_s, ghost_r, relay_s, relay_r, direct_s, direct_r, plane_ready):
    me = lax.axis_index("blk")
    lvl = lax.axis_index("lvl")
    blocks = out.shape[1]
    spread = EDGE * LANE_TILES * blocks
    pitch = (LANE_TILES + 1) * blocks
    coarse_level = jnp.maximum(lvl - 1, 0)
    fine_level = jnp.minimum(lvl + 1, levels - 1)
    pieces = [(x1 - x0) * LANE_TILES for x0, x1 in PARTS]
    wholes = (whole0, whole1, whole2, whole3)
    sends, gots = (send0, send1, send2, send3), (got0, got1, got2, got3)
    after = device(lax.rem(me + 1, n), lvl)
    before = device(lax.rem(me + n - 1, n), lvl)
    below_level = device(me, coarse_level)
    has_coarse, has_fine = lvl > 0, lvl < levels - 1
    not_first, not_last = me > 0, me < n - 1

    others = range(1, n)
    partners = [lax.rem(me + k, n) for k in range(n)]
    sources = [lax.rem(me + n - k, n) for k in range(n)]

    barrier = pltpu.get_barrier_semaphore()

    def greet(blk, level):
        pl.semaphore_signal(barrier, inc=1, device_id=device(blk, level), device_id_type=MESH)

    for k in others:
        greet(partners[k], lvl)

    @pl.when(has_fine)
    def _():
        greet(me, fine_level)

    index_loads = [
        pltpu.make_async_copy(src, dst, index_sem.at[i])
        for i, (src, dst) in enumerate(((spots_in, spots), (parents_in, parent_slot), (flags_in, flags)))
    ]
    loads = []
    for i, (lo, hi) in enumerate(PIECES):
        part = pl.ds(lo, hi - lo)
        loads.append((
            pltpu.make_async_copy(shift_in.at[:, part], field.at[3, :, part], in_sem.at[2 * i]),
            pltpu.make_async_copy(vort_in.at[:, :, part], field.at[pl.ds(0, 3), :, part], in_sem.at[2 * i + 1]),
        ))
    constants = (
        pltpu.make_async_copy(shrink_in, shrink, table_sem.at[0]),
        pltpu.make_async_copy(grow_in, grow, table_sem.at[1]),
    )
    for copy in loads[0]:
        copy.start()
    for copy in index_loads:
        copy.start()
    for copy in loads[1] + loads[2]:
        copy.start()
    for copy in constants:
        copy.start()

    sublane = lax.broadcasted_iota(jnp.int32, (blocks, 128), 0)
    lane = lax.broadcasted_iota(jnp.int32, (1, 128), 1)

    def tile(f, x, j):
        at = pl.multiple_of(x * PLANE + j * 128, 128)
        return field[f, :, pl.ds(at, 128)].astype(jnp.float32)

    def source_tile(f, x, j):
        if x < 0:
            edge_row = halo_low[pl.ds(f * 16 + (x + 2) * LANE_TILES + j, 1), :]
            return jnp.where(sublane == 0, edge_row, pltpu.roll(tile(f, x + EDGE, j), 1, 0))
        if x >= EDGE:
            edge_row = halo_high[pl.ds(f * 16 + (x - EDGE) * LANE_TILES + j, 1), :]
            return jnp.where(sublane == blocks - 1, edge_row, pltpu.roll(tile(f, x - EDGE, j), blocks - 1, 0))
        return tile(f, x, j)

    def remesh(part):
        (x0, x1), piece = PARTS[part], pieces[part]

        def chunk(j, carry):
            sums = [{}, {}, {}]
            for x in range(x0 - 2, x1 + 2):
                weights = tap_weights(source_tile(3, x, j))
                for c in range(3):
                    value = source_tile(c, x, j)
                    for offset in range(-2, 3):
                        to = x + offset
                        if x0 <= to < x1:
                            term = value * weights[offset]
                            sums[c][to] = sums[c][to] + term if to in sums[c] else term
                    if x0 <= x - 2:
                        at = c * spread + ((x - 2) * LANE_TILES + j) * blocks
                        rows[pl.ds(pl.multiple_of(at, blocks), blocks), :] = sums[c].pop(x - 2)
            return carry

        lax.fori_loop(0, LANE_TILES, chunk, 0)
        for b in range(blocks):
            for c in range(3):
                at = c * spread + x0 * LANE_TILES * blocks + b
                wholes[part][b, c * piece:(c + 1) * piece, :] = rows[
                    pl.ds(at, piece, stride=blocks), :
                ].astype(jnp.bfloat16)

    def pack(part):
        def one(to, carry):
            for s in range(CAP):
                sends[part][to, s] = wholes[part][pick[CAP * to + s]]
            return carry

        lax.fori_loop(0, n, one, 0)

    def keep(part):
        for s in range(CAP):
            gots[part][CAP * me + s] = wholes[part][pick[CAP * me + s]]

    def block_copy(part, to):
        return remote(sends[part].at[to], gots[part].at[pl.ds(CAP * me, CAP)],
                      block_s.at[part, to], block_r.at[part, me], device(to, lvl))

    def block_arrival(part, source):
        return remote(sends[part].at[me], gots[part].at[pl.ds(CAP * source, CAP)],
                      block_s.at[part, source], block_r.at[part, source], before)

    def send_blocks(part):
        for k in others:
            block_copy(part, partners[k]).start()

    def near(k):
        return remote(tab, near_tabs.at[me], near_s.at[k], near_r.at[k], device(partners[k], lvl))

    def near_arrival(k):
        return remote(tab, near_tabs.at[sources[k]], near_s.at[k], near_r.at[k], before)

    def down():
        return remote(near_tabs, fine_tabs, down_s, down_r, below_level)

    def ghost_copy(k, size):
        part = pl.ds(0, size)
        return remote(ghost.at[partners[k], :, part], relay.at[pl.ds(CAP * me, CAP), part],
                      ghost_s.at[k], ghost_r.at[k], device(partners[k], lvl))

    def ghost_arrival(k, size):
        part = pl.ds(0, size)
        return remote(ghost.at[me, :, part], relay.at[pl.ds(CAP * sources[k], CAP), part],
                      ghost_s.at[k], ghost_r.at[k], before)

    def relay_copy(k, size):
        pair, part = pl.ds(CAP * sources[k], CAP), pl.ds(0, size)
        origin = ghost.at[me, :, part] if k == 0 else relay.at[pair, part]
        return remote(origin, got_ghost.at[pair, part], relay_s.at[k], relay_r.at[k], below_level)

    def direct_copy(k, size):
        part = pl.ds(size, 96 - size)
        return remote(ghost.at[partners[k], :, part], got_ghost.at[pl.ds(CAP * me, CAP), part],
                      direct_s.at[k], direct_r.at[k], device(partners[k], coarse_level))

    def direct_arrival(k, size):
        part = pl.ds(size, 96 - size)
        return remote(ghost.at[me, :, part], got_ghost.at[pl.ds(CAP * sources[k], CAP), part],
                      direct_s.at[k], direct_r.at[k], before)

    def on_level(shift, action):
        for level in range(1, levels):
            pl.when(lvl == level - shift)(functools.partial(action, shared_rows(level, levels)))

    def high(target):
        return remote(edge_high, below, halo_s.at[0], halo_r.at[0], target)

    def low(target):
        return remote(edge_low, above, halo_s.at[1], halo_r.at[1], target)

    for copy in index_loads:
        copy.wait()
    head = jnp.zeros((1, 128), jnp.int32)
    for part, ref in enumerate((spots, parent_slot, flags)):
        for b in range(blocks):
            head = jnp.where(lane == part * blocks + b, ref[0, b], head)
    tab[...] = head
    near_tabs[me] = head
    owners = [split(spots[0, b], blocks)[0] for b in range(blocks)]

    def choose(to, carry):
        first, second = picks(owners, to)
        pick[CAP * to] = first
        pick[CAP * to + 1] = second
        return carry

    lax.fori_loop(0, n, choose, 0)

    for copy in loads[0]:
        copy.wait()
    remesh(0)
    pack(0)
    for copy in loads[1] + loads[2]:
        copy.wait()

    def edges(j, carry):
        for f in range(4):
            for p in range(2):
                at = f * 16 + p * LANE_TILES + j
                edge[pl.ds(at, 1), :] = tile(f, p, j)[0:1, :]
                edge[pl.ds(64 + at, 1), :] = tile(f, EDGE - 2 + p, j)[blocks - 1:blocks, :]
        return carry

    lax.fori_loop(0, LANE_TILES, edges, 0)
    edge_low[...] = edge[0:64, :].astype(jnp.bfloat16)
    edge_high[...] = edge[64:128, :].astype(jnp.bfloat16)

    pl.semaphore_wait(barrier, n - 1 + has_coarse.astype(jnp.int32))

    send_blocks(0)

    @pl.when(not_last)
    def _():
        high(after).start()

    @pl.when(not_first)
    def _():
        low(before).start()

    for k in others:
        near(k).start()
    keep(0)
    remesh(1)
    pack(1)
    keep(1)
    send_blocks(1)

    @pl.when(not_last)
    def _():
        low(after).wait_recv()

    @pl.when(not_first)
    def _():
        high(before).wait_recv()

    halo_low[...] = jnp.where(not_first, below[...].astype(jnp.float32), 0.0)
    halo_high[...] = jnp.where(not_last, above[...].astype(jnp.float32), 0.0)
    for part in (2, 3):
        remesh(part)
        pack(part)
        keep(part)

    for k in others:
        near_arrival(k).wait_recv()

    @pl.when(has_coarse)
    def _():
        down().start()

    fetch_near = pltpu.make_async_copy(near_tabs, near_local, table_sem.at[2])
    fetch_near.start()
    fetch_near.wait()
    for copy in constants:
        copy.wait()

    @pl.when(has_coarse)
    def _():
        parents = []
        for b in range(blocks):
            home, spot = split(spots[0, b], blocks)
            parents.append(split(near_local[home, 0, blocks + spot], 8 * blocks)[0])

        def choose_ghost(to, carry):
            first, second = picks(parents, to)
            pick_ghost[CAP * to] = first
            pick_ghost[CAP * to + 1] = second
            return carry

        lax.fori_loop(0, n, choose_ghost, 0)

        def restrict(b, carry):
            columns = []
            for half in range(2):
                for dx in range(2):
                    for odd in range(2):
                        parts = []
                        for c in range(3):
                            for jj in range(4):
                                x, j = half * 16 + dx, 2 * jj + odd
                                at = c * spread + (x * LANE_TILES + j) * blocks + b
                                parts.append(rows[pl.ds(at, 8, stride=2 * LANE_TILES * blocks), :])
                        columns.append(jnp.concatenate(parts, axis=0).astype(jnp.bfloat16))
            wide = jnp.concatenate(columns, axis=1)
            small[b] = jnp.dot(wide, shrink[...], preferred_element_type=jnp.float32).astype(jnp.bfloat16)
            return carry

        lax.fori_loop(0, blocks, restrict, 0)

        def pack_ghost(to, carry):
            for s in range(CAP):
                ghost[to, s] = small[pick_ghost[CAP * to + s]]
            return carry

        lax.fori_loop(0, n, pack_ghost, 0)

    def settle_places(source, places):
        count = jnp.int32(0)
        for b in range(blocks):
            owner, spot = split(near_local[source, 0, b], blocks)
            mine = owner == me
            slot = CAP * source + jnp.minimum(count, CAP - 1)
            places = jnp.where(lane == jnp.where(mine, spot, -1), slot, places)
            count = count + mine.astype(jnp.int32)
        return places

    line[...] = lax.fori_loop(0, n, settle_places, jnp.zeros((1, 128), jnp.int32))
    def share(size):
        for k in others:
            ghost_copy(k, size).start()
        relay_copy(0, size).start()

    on_level(0, share)
    for part in (2, 3):
        send_blocks(part)

    @pl.when(has_fine)
    def _():
        down().wait_recv()
        pl.semaphore_signal(plane_ready, inc=1, device_id=device(me, fine_level), device_id_type=MESH)
        fetch_fine = pltpu.make_async_copy(fine_tabs, fine_local, table_sem.at[4])
        fetch_fine.start()
        fetch_fine.wait()

    @pl.when(has_coarse)
    def _():
        pl.semaphore_wait(plane_ready, 1)

    def rest(size):
        for k in range(n):
            direct_copy(k, size).start()

    on_level(0, rest)
    empty = CAP * n

    def settle_octants(source, codes):
        count = jnp.int32(0)
        for b in range(blocks):
            home, spot = split(fine_local[source, 0, b], blocks)
            owner, code = split(fine_local[home, 0, blocks + spot], 8 * blocks)
            mine = owner == me
            hit = jnp.logical_and(mine, fine_local[home, 0, 2 * blocks + spot] == 1)
            slot = CAP * source + jnp.minimum(count, CAP - 1)
            codes = jnp.where(lane == jnp.where(hit, code, -1), slot, codes)
            count = count + mine.astype(jnp.int32)
        return codes

    rounds = jnp.where(has_fine, n, 0)
    line2[...] = lax.fori_loop(0, rounds, settle_octants, jnp.full((1, 128), empty, jnp.int32))
    got_ghost[empty] = jnp.zeros(got_ghost.shape[1:], jnp.bfloat16)
    fetch_place = pltpu.make_async_copy(line, place, table_sem.at[3])
    fetch_octants = pltpu.make_async_copy(line2, octants, table_sem.at[5])
    fetch_place.start()
    fetch_octants.start()
    fetch_place.wait()
    fetch_octants.wait()

    wide_lane = lax.broadcasted_iota(jnp.int32, (blocks, 128), 1)
    deep = lax.bitwise_and(wide_lane, 16) != 0
    for corner in range(4):
        mask = jnp.zeros((blocks, 128), jnp.int32)
        for q in range(blocks):
            near_half = (octants[0, q * 8 + corner * 2] < empty).astype(jnp.int32)
            far_half = (octants[0, q * 8 + corner * 2 + 1] < empty).astype(jnp.int32)
            mask = jnp.where(sublane == q, jnp.where(deep, far_half, near_half), mask)
        masks[corner] = mask

    def scatter(part):
        for k in others:
            block_arrival(part, sources[k]).wait_recv()

        piece = pieces[part]

        def one(q, carry):
            block = gots[part][place[0, q]].astype(jnp.float32)
            for c in range(3):
                at = c * spread + PARTS[part][0] * LANE_TILES * blocks + q
                rows[pl.ds(at, piece, stride=blocks), :] = block[c * piece:(c + 1) * piece, :]
            return carry

        lax.fori_loop(0, blocks, one, 0)

    def finish(part):
        def one(x, carry):
            flagged = [masks[2 * lax.div(x, 16) + oy] != 0 for oy in range(2)]
            for c in range(3):
                for j in range(LANE_TILES):
                    at = pl.multiple_of(c * spread + (x * LANE_TILES + j) * blocks, blocks)
                    over = pl.multiple_of((c * EDGE + x) * pitch + j * blocks, blocks)
                    value = jnp.where(flagged[j // 4], patch[pl.ds(over, blocks), :], rows[pl.ds(at, blocks), :])
                    to = pl.multiple_of(x * PLANE + j * 128, 128)
                    out[c, :, pl.ds(to, 128)] = value.astype(jnp.bfloat16)
            return carry

        lax.fori_loop(*PARTS[part], one, 0)

    scatter(0)
    scatter(1)

    def forward(size):
        for k in others:
            ghost_arrival(k, size).wait_recv()
            relay_copy(k, size).start()

    def gather(size):
        for k in range(n):
            relay_copy(k, size).wait_recv()
            direct_arrival(k, size).wait_recv()

    on_level(0, forward)
    scatter(2)
    on_level(1, gather)

    @pl.when(has_fine)
    def _():
        def expand(q, carry):
            pairs = []
            for corner in range(4):
                at = q * 8 + corner * 2
                pairs.append(jnp.concatenate([got_ghost[octants[0, at]], got_ghost[octants[0, at + 1]]], axis=1))
            full = jnp.dot(jnp.concatenate(pairs, axis=0), grow[...], preferred_element_type=jnp.float32)
            for corner in range(4):
                for c in range(3):
                    for jj in range(4):
                        for half in range(2):
                            x, j = corner // 2 * 16 + half * 8, corner % 2 * 4 + jj
                            to = (c * EDGE + x) * pitch + j * blocks + q
                            at = (corner * 12 + c * 4 + jj) * 8
                            patch[pl.ds(to, 8, stride=pitch), :] = full[at:at + 8, half * 128:(half + 1) * 128]
            return carry

        lax.fori_loop(0, blocks, expand, 0)

    for part in (0, 1, 2):
        finish(part)
    @pl.when(not_last)
    def _():
        high(after).wait_send()

    @pl.when(not_first)
    def _():
        low(before).wait_send()

    for k in others:
        near(k).wait_send()
        for part in (0, 1, 2):
            block_copy(part, partners[k]).wait_send()

    @pl.when(has_coarse)
    def _():
        down().wait_send()

    def drain(size):
        for k in others:
            ghost_copy(k, size).wait_send()
        for k in range(n):
            relay_copy(k, size).wait_send()
            direct_copy(k, size).wait_send()

    on_level(0, drain)

    scatter(3)
    finish(3)

    for k in others:
        block_copy(3, partners[k]).wait_send()


def selection_tables():
    k = np.arange(1024)
    half, dx, odd, y, z = k // 512, k // 256 % 2, k // 128 % 2, k % 128 // 32, k % 32
    target = half * 64 + (2 * odd + y // 2) * 16 + z // 2
    shrink = np.where(target[:, None] == np.arange(128)[None, :], 0.125, 0.0)
    k = np.arange(256)
    oz, half, y, z = k // 128, k % 128 // 64, k % 64 // 16, k % 16
    target = half * 128 + y * 32 + oz * 16 + z
    grow = np.where(target[:, None] == np.arange(256)[None, :], 1.0, 0.0)
    return shrink, grow


def body(n, levels, vorticity, shift_field, new_index, parent_slot, flags):
    blocks, cells = vorticity.shape[2:]
    vort, shift = vorticity[0], shift_field[0]
    hbm = pl.BlockSpec(memory_space=pltpu.HBM)
    vmem = pl.BlockSpec(memory_space=pltpu.VMEM)
    bf16, f32, i32 = jnp.bfloat16, jnp.float32, jnp.int32
    dma, vm, smem = pltpu.SemaphoreType.DMA, pltpu.VMEM, pltpu.SMEM
    spread = EDGE * LANE_TILES * blocks
    pieces = [3 * (x1 - x0) * LANE_TILES for x0, x1 in PARTS]
    parts = len(PARTS)
    shrink, grow = selection_tables()
    out = pl.pallas_call(
        functools.partial(kernel, n, levels),
        out_shape=jax.ShapeDtypeStruct((3, blocks, cells), bf16),
        in_specs=[hbm] * 7,
        out_specs=vmem,
        scratch_shapes=[
            smem((1, blocks), i32), smem((1, blocks), i32), smem((1, blocks), i32),
            vm((4, blocks, cells), bf16), vm(shrink.shape, bf16), vm(grow.shape, bf16),
            vm((3 * spread, 128), f32), vm((3 * EDGE * (LANE_TILES + 1) * blocks, 128), f32),
            *[vm((blocks, piece, 128), bf16) for piece in pieces], vm((4, blocks, 128), i32),
            *[vm((n, CAP, piece, 128), bf16) for piece in pieces],
            *[vm((n * CAP, piece, 128), bf16) for piece in pieces],
            vm((blocks, 96, 128), bf16), vm((n, CAP, 96, 128), bf16), vm((n * CAP, 96, 128), bf16),
            vm((n * CAP + 1, 96, 128), bf16),
            vm((128, 128), f32), vm((64, 128), bf16), vm((64, 128), bf16),
            vm((64, 128), bf16), vm((64, 128), bf16), vm((64, 128), f32), vm((64, 128), f32),
            vm((1, 128), i32), vm((n, 1, 128), i32), vm((n, 1, 128), i32),
            smem((n, 1, 128), i32), smem((n, 1, 128), i32),
            vm((1, 128), i32), smem((1, 128), i32), vm((1, 128), i32), smem((1, 128), i32),
            smem((CAP * n,), i32), smem((CAP * n,), i32),
            dma((6,)), dma((3,)), dma((6,)), dma((2,)), dma((2,)), dma((n,)), dma((n,)), dma, dma,
            dma((parts, n)), dma((parts, n)), dma((n,)), dma((n,)), dma((n,)), dma((n,)), dma((n,)), dma((n,)),
            pltpu.SemaphoreType.REGULAR,
        ],
        compiler_params=pltpu.CompilerParams(
            collective_id=0, has_side_effects=True, vmem_limit_bytes=VMEM_LIMIT
        ),
        name="move",
    )(*[
        pltpu.with_memory_space_constraint(x, pltpu.HBM)
        for x in (new_index, parent_slot, flags, vort, shift, jnp.asarray(shrink, bf16), jnp.asarray(grow, bf16))
    ])
    return out[None]


def solution(mesh):
    placed = (
        P("lvl", None, "blk", None),
        P("lvl", "blk", None),
        P("lvl", "blk"),
        P("lvl", "blk"),
        P("lvl", "blk"),
    )
    step = functools.partial(body, mesh.shape["blk"], mesh.shape["lvl"])
    return jax.shard_map(
        step, mesh=mesh, in_specs=placed, out_specs=P("lvl", None, "blk", None), check_vma=False
    )
```
